32 devices in a mesh: seq: 8 (over z, x), ch: 4 (over y, core).
Axes of the slice: x: 2, y: 2, z: 4, core: 2. Of those that a mesh axis runs over, the one named last changes fastest.
Arguments:
- values: float32 [2048, 1024], P('seq', 'ch'), may hold values from -6 to 6
- gates: float32 [2048, 1024], P('seq', 'ch'), may hold values from -6 to 6
- filter_taps: float32 [4096, 1024], P('seq', 'ch'), may hold values from -0.09375 to 0.09375
- skip: float32 [1024], P('ch'), may hold values from 0.5 to 2
- out_weight: bfloat16 [1024, 2048], P(None, 'ch'), may hold values from -0.1875 to 0.1875
Outputs:
- mixed: float32 [2048, 2048], P('seq', 'ch')
The draws below stay inside these ranges and needn't reach their ends.
All inputs are finite; a program needn't handle non-finite values.
Results may differ from the reference program's by a relative error of at most 0.0058.
Values may be sent and summed in bfloat16 or wider, within the bound.
A program may use at most 64 MiB of HBM per device.

```python
import jax
import jax.numpy as jnp

D = 2048
CHANNELS = 1024
FILTER = 4096
TOKENS = 2048


def shard_levels(key, dims, shards, low, top_value):
    factor_of, own = 1.0, jax.random.fold_in(key, 6)
    for position, parts in shards:
        steps = jnp.exp(jax.random.uniform(jax.random.fold_in(own, position), (parts,), jnp.float32, low / len(shards), top_value / len(shards)))
        factor_of = factor_of * jnp.repeat(steps, dims[position] // parts).reshape([-1 if axis == position else 1 for axis in range(len(dims))])
    return factor_of


def gaussian(rng, shape, deviation, bound, split=(), kind=jnp.bfloat16):
    loudness = shard_levels(rng, shape, split, -0.22, 0.18) if split else 1.0
    result = jax.random.normal(rng, shape, jnp.float32) * deviation * loudness
    return jnp.minimum(jnp.maximum(result, -bound), bound).astype(kind)


def setup_inputs(seed: int = 0) -> dict:
    arg_keys = jax.random.split(jax.random.key(seed), 6)
    return {
        "values": gaussian(arg_keys[0], (TOKENS, CHANNELS), 1.0, 6.0, ((0, 8), (1, 4)), jnp.float32),
        "gates": gaussian(arg_keys[1], (TOKENS, CHANNELS), 1.0, 6.0, ((0, 8), (1, 4)), jnp.float32),
        "filter_taps": gaussian(arg_keys[2], (FILTER, CHANNELS), FILTER ** -0.5, 0.09375, ((0, 8), (1, 4)), jnp.float32),
        "skip": jnp.clip(0.5 + 1.5 * jax.random.uniform(arg_keys[3], (CHANNELS,), jnp.float32) ** shard_levels(arg_keys[3], (CHANNELS,), ((0, 4),), -0.2, 0.2), 0.5, 2.0),
        "out_weight": gaussian(arg_keys[4], (CHANNELS, D), CHANNELS ** -0.5, 0.1875, ((1, 4),)),
    }


def reference(values, gates, filter_taps, skip, out_weight):
    length = values.shape[0]
    padded = 1 << (length + FILTER - 1).bit_length()
    spectrum = jnp.fft.rfft(values, n=padded, axis=0) * jnp.fft.rfft(filter_taps, n=padded, axis=0)
    convolved = jnp.fft.irfft(spectrum, n=padded, axis=0)[:length]
    hidden = (gates * (convolved + skip[None, :] * values)).astype(jnp.bfloat16)
    return jnp.dot(hidden, out_weight, preferred_element_type=jnp.float32)
```

```python
import functools
import math

import jax
import jax.numpy as jnp
import numpy as np
from jax import lax
from jax.experimental import pallas as pl
from jax.experimental.pallas import tpu as pltpu
from jax.sharding import PartitionSpec as P

HIGHEST = lax.Precision.HIGHEST
MESH = pl.DeviceIdType.MESH
LANES = 128
TILE = 16
PAIR = 2


def split_length(length):
    leading = 1
    for factor in range(1, math.isqrt(length) + 1):
        if length % factor == 0:
            leading = factor
    return (leading, length // leading)


def phase_table(count_rows, count_cols, modulus):
    row_ids = jnp.arange(count_rows, dtype=jnp.int32)
    col_ids = jnp.arange(count_cols, dtype=jnp.int32)
    wrapped = row_ids[:, None] * col_ids[None, :] % modulus
    phases = 2.0 * math.pi / modulus * wrapped.astype(jnp.float32)
    return (jnp.cos(phases), jnp.sin(phases))


def complex_form(cosine, sine):
    upper = jnp.stack([cosine, -sine], axis=1)
    lower = jnp.stack([sine, cosine], axis=1)
    return jnp.stack([upper, lower], axis=0)


def transform_tables(length):
    rows_lead, rows_tail = split_length(length)
    cos_lead, sin_lead = phase_table(rows_lead, rows_lead, rows_lead)
    cos_tail, sin_tail = phase_table(rows_tail, rows_tail, rows_tail)
    cos_twist, sin_twist = phase_table(rows_lead, rows_tail, length)
    lead_table = jnp.stack([cos_lead, -sin_lead])
    tail_forward = complex_form(cos_tail, -sin_tail)
    tail_inverse = complex_form(cos_tail, sin_tail)
    return (
        lead_table,
        tail_forward,
        tail_inverse,
        cos_twist,
        sin_twist,
        rows_lead,
        rows_tail,
        length,
    )


def twist_rows(section, cosine, sine):
    real_part = section[0] * cosine[None] - section[1] * sine[None]
    imag_part = section[0] * sine[None] + section[1] * cosine[None]
    return jnp.stack([real_part, imag_part])


def forward_rows(rows, tables):
    lead_table, tail_forward, tail_inverse, cos_twist, sin_twist, rows_lead, rows_tail, length = (
        tables
    )
    signal = jnp.concatenate([rows, jnp.zeros_like(rows)], axis=1).reshape(
        rows.shape[0], rows_lead, rows_tail
    )
    section = jnp.einsum("pft,cts->pcfs", lead_table, signal, precision=HIGHEST)
    twisted = twist_rows(section, cos_twist, -sin_twist)
    return jnp.einsum("pgrs,rcfs->pcfg", tail_forward, twisted, precision=HIGHEST)


def inverse_rows(spectrum, tables):
    lead_table, tail_forward, tail_inverse, cos_twist, sin_twist, rows_lead, rows_tail, length = (
        tables
    )
    section = jnp.einsum("pgrs,rcfs->pcfg", tail_inverse, spectrum, precision=HIGHEST)
    twisted = twist_rows(section, cos_twist, sin_twist)
    signal = jnp.einsum("rft,rcfs->cts", lead_table, twisted, precision=HIGHEST) / length
    return signal.reshape(signal.shape[0], length)


def product(left, right):
    real_part = left[0] * right[0] - left[1] * right[1]
    imag_part = left[0] * right[1] + left[1] * right[0]
    return jnp.stack([real_part, imag_part])


def body(values, gates, filter_taps, skip, out_weight):
    block_rows, width = values.shape
    whole_filter = lax.all_gather(filter_taps, "seq", axis=0, tiled=True)
    devices = lax.axis_size("seq")
    narrow = width // devices
    whole_rows = lax.all_to_all(values.T, "seq", split_axis=0, concat_axis=1, tiled=True)
    total_rows = whole_rows.shape[1]
    own_taps = lax.dynamic_slice_in_dim(whole_filter, lax.axis_index("seq") * narrow, narrow, 1).T
    used_taps = min(own_taps.shape[1], total_rows)
    own_taps = own_taps[:, :used_taps]
    taps_rows = jnp.concatenate(
        [own_taps, jnp.zeros((narrow, total_rows - used_taps), jnp.float32)], axis=1
    )
    row_tables = transform_tables(2 * total_rows)
    spectrum = product(forward_rows(whole_rows, row_tables), forward_rows(taps_rows, row_tables))
    convolved_rows = inverse_rows(spectrum, row_tables)[:, :total_rows]
    convolved = lax.all_to_all(convolved_rows, "seq", split_axis=1, concat_axis=0, tiled=True).T
    hidden = (gates * (convolved + skip[None, :] * values)).astype(jnp.bfloat16)
    return jnp.dot(
        lax.all_gather(hidden, "ch", axis=1, tiled=True),
        out_weight,
        preferred_element_type=jnp.float32,
    )


def block_tables():
    size = 2 * LANES
    place = np.arange(size)[:, None]
    odd = 2 * np.arange(LANES)[None, :] + 1
    angle = np.pi / size * (place * odd % (2 * size))
    forward = np.concatenate([np.cos(angle), -np.sin(angle)], axis=1)
    inverse = forward[LANES:].T / LANES

    def two_parts(table, axis):
        high = table.astype(jnp.bfloat16)
        low = (table - high.astype(np.float64)).astype(jnp.bfloat16)
        return np.concatenate([high, low], axis=axis)

    return two_parts(forward, 0), two_parts(inverse, 1)


def block_kernel(
    tap_sources,
    values_hbm,
    gates_hbm,
    taps_hbm,
    skip_ref,
    weight_hbm,
    forward_hbm,
    inverse_hbm,
    out_hbm,
    values_ref,
    gates_ref,
    taps_ref,
    out_ref,
    x_out,
    h_out,
    x_in,
    h_in,
    x_waves,
    h_waves,
    y_waves,
    y_out,
    y_in,
    hidden,
    weight,
    forward,
    inverse,
    load_sem,
    out_sem,
    x_send,
    x_recv,
    h_send,
    h_recv,
    y_send,
    y_recv,
    g_send,
    g_recv,
):
    seq_size, narrow, block_rows = x_out.shape
    tap_rows = h_out.shape[2]
    ch_size, _, width = hidden.shape
    per = block_rows // LANES
    me, lane_group = lax.axis_index("seq"), lax.axis_index("ch")
    f32, bf16 = jnp.float32, jnp.bfloat16

    loads = [
        pltpu.make_async_copy(source, target, load_sem.at[place])
        for place, (source, target) in enumerate(
            (
                (values_hbm, values_ref),
                (taps_hbm, taps_ref),
                (forward_hbm, forward),
                (inverse_hbm, inverse),
                (gates_hbm, gates_ref),
                (weight_hbm, weight),
            )
        )
    ]
    for load in loads:
        load.start()

    barrier = pltpu.get_barrier_semaphore()
    for step in range(1, seq_size):
        pl.semaphore_signal(
            barrier, inc=1, device_id={"seq": lax.rem(me + step, seq_size)}, device_id_type=MESH
        )
    for step in range(1, ch_size):
        pl.semaphore_signal(
            barrier, inc=1, device_id={"ch": lax.rem(lane_group + step, ch_size)}, device_id_type=MESH
        )

    loads[0].wait()
    x_out[...] = values_ref[...].T.astype(bf16).reshape(x_out.shape)
    x_in[me] = x_out[me]
    loads[1].wait()

    @pl.when(me < tap_sources)
    def _():
        h_out[...] = taps_ref[...].T.astype(bf16).reshape(h_out.shape)
        h_in[me] = h_out[me]

    rounds = seq_size // PAIR
    home, side = me // PAIR, lax.rem(me, PAIR)
    targets = []
    for near in [rounds // 2] + [n for k in range(1, (rounds + 1) // 2) for n in (rounds - k, k)] + [0]:
        for turn in range(PAIR):
            if near or turn:
                targets.append(
                    lax.rem(home + near, rounds) * PAIR + lax.rem(side + turn, PAIR)
                )

    def x_copy(place, to):
        return pltpu.make_async_remote_copy(
            x_out.at[to], x_in.at[me], x_send.at[place], x_recv.at[me],
            device_id={"seq": to}, device_id_type=MESH,
        )

    def h_copy(place, to):
        return pltpu.make_async_remote_copy(
            h_out.at[to], h_in.at[me], h_send.at[place], h_recv.at[me],
            device_id={"seq": to}, device_id_type=MESH,
        )

    pl.semaphore_wait(barrier, seq_size + ch_size - 2)
    x_copies = [x_copy(place, to) for place, to in enumerate(targets)]
    for copy in x_copies:
        copy.start()

    @pl.when(me < tap_sources)
    def _():
        for place, to in enumerate(targets):
            h_copy(place, to).start()

    for load in loads[2:4]:
        load.wait()

    def take_taps(source):
        @pl.when(me != source)
        def _():
            pltpu.make_async_remote_copy(
                h_out.at[0], h_in.at[source], h_send.at[0], h_recv.at[source],
                device_id={"seq": source}, device_id_type=MESH,
            ).wait_recv()
        pieces = tap_rows // LANES
        rows = jnp.concatenate(
            [h_in[source, :, piece * LANES : (piece + 1) * LANES] for piece in range(pieces)], axis=0
        )
        table = jnp.concatenate(
            [forward[:LANES], forward[2 * LANES : 3 * LANES]], axis=0
        )
        waves = jnp.dot(
            jnp.concatenate([rows, rows], axis=1), table, preferred_element_type=f32
        )
        h_waves[source * pieces : (source + 1) * pieces] = waves.reshape(
            pieces, narrow, 2 * LANES
        )

    def take_values(first):
        for source in range(first, first + PAIR):
            @pl.when(me != source)
            def _():
                pltpu.make_async_remote_copy(
                    x_out.at[0], x_in.at[source], x_send.at[0], x_recv.at[source],
                    device_id={"seq": source}, device_id_type=MESH,
                ).wait_recv()
        if first:
            before = x_in[first - 1, :, block_rows - LANES :]
        else:
            before = jnp.zeros((narrow, LANES), bf16)
        rows = []
        for source in range(first, first + PAIR):
            for piece in range(per):
                here = x_in[source, :, piece * LANES : (piece + 1) * LANES]
                rows.append(jnp.concatenate([before, here, before, here], axis=1))
                before = here
        waves = jnp.dot(
            jnp.concatenate(rows, axis=0), forward[...], preferred_element_type=f32
        )
        x_waves[first * per : (first + PAIR) * per] = waves.reshape(
            PAIR * per, narrow, 2 * LANES
        )

    def multiply(first):
        start = first * per
        count = PAIR * per
        for part in range(narrow // TILE):
            rows = slice(part * TILE, (part + 1) * TILE)
            cache = {}

            def x_part(block):
                if block not in cache:
                    cache[block] = (x_waves[block, rows, :LANES], x_waves[block, rows, LANES:])
                return cache[block]

            sums = [None] * count
            for lag in range(start + count):
                h_real, h_imag = h_waves[lag, rows, :LANES], h_waves[lag, rows, LANES:]
                for spot in range(count):
                    block = start + spot - lag
                    if block < 0:
                        continue
                    x_real, x_imag = x_part(block)
                    real = x_real * h_real - x_imag * h_imag
                    imag = x_real * h_imag + x_imag * h_real
                    if sums[spot] is None:
                        sums[spot] = (real, imag)
                    else:
                        sums[spot] = (sums[spot][0] + real, sums[spot][1] + imag)
            for spot in range(count):
                y_waves[spot, rows, :LANES] = sums[spot][0]
                y_waves[spot, rows, LANES:] = sums[spot][1]

    def y_copy(target, piece):
        span = pl.ds(piece * LANES, LANES)
        return pltpu.make_async_remote_copy(
            y_out.at[target, :, span], y_in.at[me, :, span],
            y_send.at[target, piece], y_recv.at[me, piece],
            device_id={"seq": target}, device_id_type=MESH,
        )

    def give_back(first):
        waves = y_waves[...].reshape(PAIR * per * narrow, 2 * LANES)
        high = waves.astype(bf16)
        low = (waves - high.astype(f32)).astype(bf16)
        both = jnp.dot(high, inverse[...], preferred_element_type=f32)
        rest = jnp.dot(low, inverse[:, :LANES], preferred_element_type=f32)
        convolved = (both[:, :LANES] + both[:, LANES:] + rest).astype(bf16)
        for spot in range(PAIR * per):
            source, piece = first + spot // per, spot % per
            y_out[source, :, piece * LANES : (piece + 1) * LANES] = convolved[
                spot * narrow : (spot + 1) * narrow
            ]
        for piece in range(per):
            for target in range(first, first + PAIR):
                @pl.when(me != target)
                def _():
                    y_copy(target, piece).start()

    taken = 0
    for first in range(0, seq_size, PAIR):
        while taken < tap_sources and taken * tap_rows < (first + PAIR) * block_rows:
            take_taps(taken)
            taken += 1
        take_values(first)
        multiply(first)
        give_back(first)
    y_in[me] = y_out[me]

    partner = lane_group + 1 - 2 * lax.rem(lane_group, 2)
    pairs = ch_size // 2

    def spread(kind, piece, slot, to):
        block = hidden.at[slot, pl.ds(piece * LANES, LANES)]
        copy = pltpu.make_async_remote_copy(
            block, block, g_send.at[kind, piece], g_recv.at[kind, piece],
            device_id={"ch": to}, device_id_type=MESH,
        )
        copy.start()
        g_copies.append(copy)
        return copy

    def add_product(piece, slot, first=False):
        rows = slice(piece * LANES, (piece + 1) * LANES)
        term = jnp.dot(hidden[slot, rows], weight[slot], preferred_element_type=f32)
        out_ref[rows] = term if first else out_ref[rows] + term

    g_copies, direct, relayed = [], {}, {}
    loads[4].wait()
    for piece in range(per):
        rows = slice(piece * LANES, (piece + 1) * LANES)
        for source in range(seq_size):
            @pl.when(me != source)
            def _():
                span = pl.ds(piece * LANES, LANES)
                pltpu.make_async_remote_copy(
                    y_out.at[source, :, span], y_in.at[source, :, span],
                    y_send.at[source, piece], y_recv.at[source, piece],
                    device_id={"seq": source}, device_id_type=MESH,
                ).wait_recv()
        convolved = y_in[:, :, rows].astype(f32).reshape(width, LANES).T
        hidden[lane_group, rows] = (
            gates_ref[rows] * (convolved + skip_ref[...] * values_ref[rows])
        ).astype(bf16)
        for pair in range(1, pairs):
            direct[pair, piece] = spread(
                2 * pair - 1, piece, lane_group, lax.rem(lane_group + 2 * pair, ch_size)
            )
        direct[0, piece] = spread(0, piece, lane_group, partner)
    loads[5].wait()
    for piece in range(per):
        add_product(piece, lane_group, True)
    for piece in range(per):
        direct[0, piece].wait_recv()
        add_product(piece, partner)
    for piece in range(per):
        for pair in range(1, pairs):
            slot = lax.rem(lane_group + ch_size - 2 * pair, ch_size)
            direct[pair, piece].wait_recv()
            relayed[pair, piece] = spread(2 * pair, piece, slot, partner)
            add_product(piece, slot)
    stores = []
    for piece in range(per):
        rows = pl.ds(piece * LANES, LANES)
        for pair in range(1, pairs):
            slot = lax.rem(partner + ch_size - 2 * pair, ch_size)
            relayed[pair, piece].wait_recv()
            add_product(piece, slot)
        store = pltpu.make_async_copy(out_ref.at[rows], out_hbm.at[rows], out_sem.at[piece])
        store.start()
        stores.append(store)
    for store in stores:
        store.wait()

    for copy in x_copies + g_copies:
        copy.wait_send()
    for target in range(seq_size):
        @pl.when(me != target)
        def _():
            for piece in range(per):
                y_copy(target, piece).wait_send()

    @pl.when(me < tap_sources)
    def _():
        for place, to in enumerate(targets):
            h_copy(place, to).wait_send()


def block_body(values, gates, filter_taps, skip, out_weight):
    seq_size, ch_size = lax.axis_size("seq"), lax.axis_size("ch")
    block_rows, width = values.shape
    tap_rows = filter_taps.shape[0]
    narrow = width // seq_size
    total = block_rows * seq_size
    sources = min(tap_rows * seq_size, total) // tap_rows
    columns = out_weight.shape[1]
    f32, bf16 = jnp.float32, jnp.bfloat16
    vmem = pl.BlockSpec(memory_space=pltpu.VMEM)
    hbm = pl.BlockSpec(memory_space=pl.ANY)
    per = block_rows // LANES
    dma = pltpu.SemaphoreType.DMA
    forward, inverse = block_tables()
    return pl.pallas_call(
        functools.partial(block_kernel, sources),
        out_shape=jax.ShapeDtypeStruct((block_rows, columns), f32),
        in_specs=[hbm] * 3 + [vmem] + [hbm] * 3,
        out_specs=hbm,
        scratch_shapes=[
            pltpu.VMEM((block_rows, width), f32),
            pltpu.VMEM((block_rows, width), f32),
            pltpu.VMEM((tap_rows, width), f32),
            pltpu.VMEM((block_rows, columns), f32),
            pltpu.VMEM((seq_size, narrow, block_rows), bf16),
            pltpu.VMEM((seq_size, narrow, tap_rows), bf16),
            pltpu.VMEM((seq_size, narrow, block_rows), bf16),
            pltpu.VMEM((sources, narrow, tap_rows), bf16),
            pltpu.VMEM((total // LANES, narrow, 2 * LANES), f32),
            pltpu.VMEM((total // LANES, narrow, 2 * LANES), f32),
            pltpu.VMEM((PAIR * per, narrow, 2 * LANES), f32),
            pltpu.VMEM((seq_size, narrow, block_rows), bf16),
            pltpu.VMEM((seq_size, narrow, block_rows), bf16),
            pltpu.VMEM((ch_size, block_rows, width), bf16),
            pltpu.VMEM((ch_size, width, columns), bf16),
            pltpu.VMEM(forward.shape, bf16),
            pltpu.VMEM(inverse.shape, bf16),
            dma((6,)),
            dma((per,)),
            dma((seq_size,)),
            dma((seq_size,)),
            dma((seq_size,)),
            dma((sources,)),
            dma((seq_size, per)),
            dma((seq_size, per)),
            dma((ch_size, per)),
            dma((ch_size, per)),
        ],
        compiler_params=pltpu.CompilerParams(
            collective_id=0, has_side_effects=True, vmem_limit_bytes=63000 * 1024
        ),
    )(
        values,
        gates,
        filter_taps,
        skip.reshape(1, width),
        out_weight.reshape(ch_size, width, columns),
        jnp.asarray(forward),
        jnp.asarray(inverse),
    )


def local_body(values, gates, filter_taps, skip, out_weight):
    seq_size = lax.axis_size("seq")
    block_rows, width = values.shape
    tap_rows = filter_taps.shape[0]
    narrow = width // seq_size
    total = block_rows * seq_size
    fits = (
        width % (seq_size * TILE) == 0
        and lax.axis_size("ch") % 2 == 0
        and width % LANES == 0
        and block_rows % LANES == 0
        and lax.axis_size("seq") % PAIR == 0
        and tap_rows % LANES == 0
        and total % tap_rows == 0
        and tap_rows % block_rows == 0
        and narrow * total <= 128 * 1024
    )
    chosen = block_body if fits else body
    return chosen(values, gates, filter_taps, skip, out_weight)


def solution(mesh):
    placed = (P("seq", "ch"), P("seq", "ch"), P("seq", "ch"), P("ch"), P(None, "ch"))
    return jax.shard_map(
        local_body, mesh=mesh, in_specs=placed, out_specs=P("seq", "ch"), check_vma=False
    )
```

```python
import functools
import math

import jax
import jax.numpy as jnp
import numpy as np
from jax import lax
from jax.experimental import pallas as pl
from jax.experimental.pallas import tpu as pltpu
from jax.sharding import PartitionSpec as P

HIGHEST = lax.Precision.HIGHEST
MESH = pl.DeviceIdType.MESH
LANES = 128
TILE = 16
PAIR = 2


def split_length(length):
    leading = 1
    for factor in range(1, math.isqrt(length) + 1):
        if length % factor == 0:
            leading = factor
    return (leading, length // leading)


def phase_table(count_rows, count_cols, modulus):
    row_ids = jnp.arange(count_rows, dtype=jnp.int32)
    col_ids = jnp.arange(count_cols, dtype=jnp.int32)
    wrapped = row_ids[:, None] * col_ids[None, :] % modulus
    phases = 2.0 * math.pi / modulus * wrapped.astype(jnp.float32)
    return (jnp.cos(phases), jnp.sin(phases))


def complex_form(cosine, sine):
    upper = jnp.stack([cosine, -sine], axis=1)
    lower = jnp.stack([sine, cosine], axis=1)
    return jnp.stack([upper, lower], axis=0)


def transform_tables(length):
    rows_lead, rows_tail = split_length(length)
    cos_lead, sin_lead = phase_table(rows_lead, rows_lead, rows_lead)
    cos_tail, sin_tail = phase_table(rows_tail, rows_tail, rows_tail)
    cos_twist, sin_twist = phase_table(rows_lead, rows_tail, length)
    lead_table = jnp.stack([cos_lead, -sin_lead])
    tail_forward = complex_form(cos_tail, -sin_tail)
    tail_inverse = complex_form(cos_tail, sin_tail)
    return (
        lead_table,
        tail_forward,
        tail_inverse,
        cos_twist,
        sin_twist,
        rows_lead,
        rows_tail,
        length,
    )


def twist_rows(section, cosine, sine):
    real_part = section[0] * cosine[None] - section[1] * sine[None]
    imag_part = section[0] * sine[None] + section[1] * cosine[None]
    return jnp.stack([real_part, imag_part])


def forward_rows(rows, tables):
    lead_table, tail_forward, tail_inverse, cos_twist, sin_twist, rows_lead, rows_tail, length = (
        tables
    )
    signal = jnp.concatenate([rows, jnp.zeros_like(rows)], axis=1).reshape(
        rows.shape[0], rows_lead, rows_tail
    )
    section = jnp.einsum("pft,cts->pcfs", lead_table, signal, precision=HIGHEST)
    twisted = twist_rows(section, cos_twist, -sin_twist)
    return jnp.einsum("pgrs,rcfs->pcfg", tail_forward, twisted, precision=HIGHEST)


def inverse_rows(spectrum, tables):
    lead_table, tail_forward, tail_inverse, cos_twist, sin_twist, rows_lead, rows_tail, length = (
        tables
    )
    section = jnp.einsum("pgrs,rcfs->pcfg", tail_inverse, spectrum, precision=HIGHEST)
    twisted = twist_rows(section, cos_twist, sin_twist)
    signal = jnp.einsum("rft,rcfs->cts", lead_table, twisted, precision=HIGHEST) / length
    return signal.reshape(signal.shape[0], length)


def product(left, right):
    real_part = left[0] * right[0] - left[1] * right[1]
    imag_part = left[0] * right[1] + left[1] * right[0]
    return jnp.stack([real_part, imag_part])


def body(values, gates, filter_taps, skip, out_weight):
    block_rows, width = values.shape
    whole_filter = lax.all_gather(filter_taps, "seq", axis=0, tiled=True)
    devices = lax.axis_size("seq")
    narrow = width // devices
    whole_rows = lax.all_to_all(values.T, "seq", split_axis=0, concat_axis=1, tiled=True)
    total_rows = whole_rows.shape[1]
    own_taps = lax.dynamic_slice_in_dim(whole_filter, lax.axis_index("seq") * narrow, narrow, 1).T
    used_taps = min(own_taps.shape[1], total_rows)
    own_taps = own_taps[:, :used_taps]
    taps_rows = jnp.concatenate(
        [own_taps, jnp.zeros((narrow, total_rows - used_taps), jnp.float32)], axis=1
    )
    row_tables = transform_tables(2 * total_rows)
    spectrum = product(forward_rows(whole_rows, row_tables), forward_rows(taps_rows, row_tables))
    convolved_rows = inverse_rows(spectrum, row_tables)[:, :total_rows]
    convolved = lax.all_to_all(convolved_rows, "seq", split_axis=1, concat_axis=0, tiled=True).T
    hidden = (gates * (convolved + skip[None, :] * values)).astype(jnp.bfloat16)
    return jnp.dot(
        lax.all_gather(hidden, "ch", axis=1, tiled=True),
        out_weight,
        preferred_element_type=jnp.float32,
    )


def block_tables():
    size = 2 * LANES
    place = np.arange(size)[:, None]
    odd = 2 * np.arange(LANES)[None, :] + 1
    angle = np.pi / size * (place * odd % (2 * size))
    forward = np.concatenate([np.cos(angle), -np.sin(angle)], axis=1)
    inverse = forward[LANES:].T / LANES

    def two_parts(table, axis):
        high = table.astype(jnp.bfloat16)
        low = (table - high.astype(np.float64)).astype(jnp.bfloat16)
        return np.concatenate([high, low], axis=axis)

    return two_parts(forward, 0), two_parts(inverse, 1)


def block_kernel(
    values_hbm,
    gates_hbm,
    taps_hbm,
    skip_ref,
    weight_hbm,
    forward_hbm,
    inverse_hbm,
    out_hbm,
    values_ref,
    gates_ref,
    taps_ref,
    out_ref,
    x_out,
    h_out,
    x_in,
    h_in,
    x_waves,
    h_waves,
    y_waves,
    y_out,
    y_in,
    hidden,
    weight,
    forward,
    inverse,
    load_sem,
    out_sem,
    x_send,
    x_recv,
    h_send,
    h_recv,
    y_send,
    y_recv,
    g_send,
    g_recv,
    seq_ready,
    ch_ready,
):
    sources, narrow, block_rows = x_out.shape
    seq_size = x_in.shape[0]
    tap_rows = h_out.shape[2]
    ch_size, halves, _, half_width = hidden.shape
    per, pieces = block_rows // LANES, tap_rows // LANES
    me, lane_group = lax.axis_index("seq"), lax.axis_index("ch")
    f32, bf16 = jnp.float32, jnp.bfloat16

    loads = [
        pltpu.make_async_copy(source, target, load_sem.at[place])
        for place, (source, target) in enumerate(
            (
                (values_hbm, values_ref),
                (taps_hbm, taps_ref),
                (forward_hbm, forward),
                (inverse_hbm, inverse),
                (gates_hbm, gates_ref),
                (weight_hbm, weight),
            )
        )
    ]
    for load in loads:
        load.start()

    barrier = pltpu.get_barrier_semaphore()
    for other in range(1, seq_size):
        @pl.when((me < other) & (me < sources))
        def _():
            pl.semaphore_signal(barrier, inc=1, device_id={"seq": other}, device_id_type=MESH)
    for other in range(1, ch_size):
        @pl.when(lane_group < other)
        def _():
            pl.semaphore_signal(barrier, inc=1, device_id={"ch": other}, device_id_type=MESH)
    earlier = jnp.minimum(me, sources) + lane_group

    @pl.when(earlier > 0)
    def _():
        pl.semaphore_wait(barrier, earlier)
    for other in range(sources):
        @pl.when(me > other)
        def _():
            pl.semaphore_signal(
                seq_ready.at[me], inc=1, device_id={"seq": other}, device_id_type=MESH
            )
    for other in range(ch_size - 1):
        @pl.when(lane_group > other)
        def _():
            pl.semaphore_signal(
                ch_ready.at[lane_group], inc=1, device_id={"ch": other}, device_id_type=MESH
            )

    def x_copy(to):
        return pltpu.make_async_remote_copy(
            x_out.at[to], x_in.at[me], x_send.at[to], x_recv.at[me],
            device_id={"seq": to}, device_id_type=MESH,
        )

    def h_copy(to):
        return pltpu.make_async_remote_copy(
            h_out.at[to], h_in.at[me], h_send.at[to], h_recv.at[me],
            device_id={"seq": to}, device_id_type=MESH,
        )

    def y_copy(to):
        return pltpu.make_async_remote_copy(
            y_out.at[to], y_in.at[me], y_send.at[to], y_recv.at[me],
            device_id={"seq": to}, device_id_type=MESH,
        )

    loads[0].wait()
    x_out[...] = values_ref[...].T.astype(bf16).reshape(x_out.shape)
    loads[1].wait()

    @pl.when(me >= sources)
    def _():
        for to in range(sources):
            x_copy(to).start()

    for load in loads[2:4]:
        load.wait()

    def take_taps(source):
        @pl.when(me != source)
        def _():
            pltpu.make_async_remote_copy(
                h_out.at[0], h_in.at[source], h_send.at[0], h_recv.at[source],
                device_id={"seq": source}, device_id_type=MESH,
            ).wait_recv()
        rows = jnp.concatenate(
            [h_in[source, :, piece * LANES : (piece + 1) * LANES] for piece in range(pieces)], axis=0
        )
        table = jnp.concatenate(
            [forward[:LANES], forward[2 * LANES : 3 * LANES]], axis=0
        )
        waves = jnp.dot(
            jnp.concatenate([rows, rows], axis=1), table, preferred_element_type=f32
        )
        h_waves[source * pieces : (source + 1) * pieces] = waves.reshape(
            pieces, narrow, 2 * LANES
        )

    def take_values(first):
        for source in range(first, first + PAIR):
            @pl.when(me != source)
            def _():
                pltpu.make_async_remote_copy(
                    x_out.at[0], x_in.at[source], x_send.at[0], x_recv.at[source],
                    device_id={"seq": 0}, device_id_type=MESH,
                ).wait_recv()
        if first:
            before = x_in[first - 1, :, block_rows - LANES :]
        else:
            before = jnp.zeros((narrow, LANES), bf16)
        rows = []
        for source in range(first, first + PAIR):
            for piece in range(per):
                here = x_in[source, :, piece * LANES : (piece + 1) * LANES]
                rows.append(jnp.concatenate([before, here, before, here], axis=1))
                before = here
        waves = jnp.dot(
            jnp.concatenate(rows, axis=0), forward[...], preferred_element_type=f32
        )
        x_waves[first * per : (first + PAIR) * per] = waves.reshape(
            PAIR * per, narrow, 2 * LANES
        )

    def multiply(first, low, high, fresh):
        start, count = first * per, PAIR * per

        def one(part, carry):
            rows = pl.ds(pl.multiple_of(part * TILE, TILE), TILE)
            real_lanes, imag_lanes = slice(0, LANES), slice(LANES, 2 * LANES)
            cache = {}

            def x_part(block):
                if block not in cache:
                    cache[block] = (
                        x_waves[block, rows, real_lanes], x_waves[block, rows, imag_lanes]
                    )
                return cache[block]

            sums = [None] * count
            if not fresh:
                sums = [
                    (y_waves[spot, rows, real_lanes], y_waves[spot, rows, imag_lanes])
                    for spot in range(count)
                ]
            for lag in range(max(0, start - high + 1), start + count - low):
                h_real, h_imag = h_waves[lag, rows, real_lanes], h_waves[lag, rows, imag_lanes]
                for spot in range(count):
                    block = start + spot - lag
                    if not low <= block < high:
                        continue
                    x_real, x_imag = x_part(block)
                    real = x_real * h_real - x_imag * h_imag
                    imag = x_real * h_imag + x_imag * h_real
                    if sums[spot] is not None:
                        real, imag = sums[spot][0] + real, sums[spot][1] + imag
                    sums[spot] = (real, imag)
            for spot in range(count):
                y_waves[spot, rows, real_lanes] = sums[spot][0]
                y_waves[spot, rows, imag_lanes] = sums[spot][1]
            return carry

        lax.fori_loop(0, narrow // TILE, one, 0)

    def give_back(first):
        waves = y_waves[...].reshape(PAIR * per * narrow, 2 * LANES)
        high = waves.astype(bf16)
        low = (waves - high.astype(f32)).astype(bf16)
        both = jnp.dot(high, inverse[...], preferred_element_type=f32)
        rest = jnp.dot(low, inverse[:, :LANES], preferred_element_type=f32)
        convolved = (both[:, :LANES] + both[:, LANES:] + rest).astype(bf16)
        for spot in range(PAIR * per):
            source, piece = first + spot // per, spot % per
            y_out[source, :, piece * LANES : (piece + 1) * LANES] = convolved[
                spot * narrow : (spot + 1) * narrow
            ]
        for to in range(first, first + PAIR):
            if to >= sources:
                pl.semaphore_wait(seq_ready.at[to], 1)

            @pl.when(me != to)
            def _():
                y_copy(to).start()

    @pl.when(me < sources)
    def _():
        h_out[...] = taps_ref[...].T.astype(bf16).reshape(h_out.shape)
        for to in range(sources):
            @pl.when(me < to)
            def _():
                pl.semaphore_wait(seq_ready.at[to], 1)

            @pl.when(me != to)
            def _():
                x_copy(to).start()
                h_copy(to).start()
        x_in[me] = x_out[me]
        h_in[me] = h_out[me]
        taken = 0
        for first in range(0, seq_size, PAIR):
            while taken < sources and taken * tap_rows < (first + PAIR) * block_rows:
                take_taps(taken)
                taken += 1
            if first:
                multiply(first, 0, first * per, True)
            take_values(first)
            multiply(first, first * per, (first + PAIR) * per, not first)
            give_back(first)
        y_in[me] = y_out[me]

    partner = lane_group + 1 - 2 * lax.rem(lane_group, 2)
    pairs = ch_size // 2
    lead = lax.rem((me // PAIR + 1) // 2, halves)
    order = [lax.rem(lead + turn, halves) for turn in range(halves)]

    def spread(kind, half, slot, to):
        block = hidden.at[slot, half]
        copy = pltpu.make_async_remote_copy(
            block, block, g_send.at[kind, half], g_recv.at[kind, half],
            device_id={"ch": to}, device_id_type=MESH,
        )
        copy.start()
        g_copies.append(copy)
        return copy

    def add_product(half, slot, first=False):
        term = jnp.dot(hidden[slot, half], weight[slot, half], preferred_element_type=f32)
        out_ref[...] = term if first else out_ref[...] + term

    for other in range(1, ch_size):
        @pl.when(lane_group < other)
        def _():
            pl.semaphore_wait(ch_ready.at[other], 1)

    g_copies, direct, relayed = [], {}, {}
    loads[4].wait()
    for turn, half in enumerate(order):
        for part in range(PAIR):
            source = half * PAIR + part

            @pl.when(me != source)
            def _():
                pltpu.make_async_remote_copy(
                    y_out.at[0], y_in.at[source], y_send.at[0], y_recv.at[source],
                    device_id={"seq": 0}, device_id_type=MESH,
                ).wait_recv()
        convolved = y_in[pl.ds(half * PAIR, PAIR)].astype(f32).reshape(half_width, block_rows).T
        span = pl.ds(pl.multiple_of(half * half_width, half_width), half_width)
        hidden[lane_group, half] = (
            gates_ref[:, span] * (convolved + skip_ref[:, span] * values_ref[:, span])
        ).astype(bf16)
        for pair in range(1, pairs):
            direct[pair, turn] = spread(
                2 * pair - 1, half, lane_group, lax.rem(lane_group + 2 * pair, ch_size)
            )
        direct[0, turn] = spread(0, half, lane_group, partner)
    loads[5].wait()
    for turn, half in enumerate(order):
        add_product(half, lane_group, not turn)
    for turn, half in enumerate(order):
        direct[0, turn].wait_recv()
        add_product(half, partner)
        for pair in range(1, pairs):
            slot = lax.rem(lane_group + ch_size - 2 * pair, ch_size)
            direct[pair, turn].wait_recv()
            relayed[pair, turn] = spread(2 * pair, half, slot, partner)
            add_product(half, slot)
    for turn, half in enumerate(order):
        for pair in range(1, pairs):
            slot = lax.rem(partner + ch_size - 2 * pair, ch_size)
            relayed[pair, turn].wait_recv()
            add_product(half, slot)
    store = pltpu.make_async_copy(out_ref, out_hbm, out_sem)
    store.start()
    store.wait()

    for copy in g_copies:
        copy.wait_send()
    for to in range(sources):
        @pl.when(me != to)
        def _():
            x_copy(to).wait_send()

        @pl.when((me != to) & (me < sources))
        def _():
            h_copy(to).wait_send()
    for to in range(seq_size):
        @pl.when((me != to) & (me < sources))
        def _():
            y_copy(to).wait_send()


def block_body(values, gates, filter_taps, skip, out_weight):
    seq_size, ch_size = lax.axis_size("seq"), lax.axis_size("ch")
    block_rows, width = values.shape
    tap_rows = filter_taps.shape[0]
    total = block_rows * seq_size
    sources = min(tap_rows * seq_size, total) // tap_rows
    narrow, halves = width // sources, sources // PAIR
    half_width = width // halves
    columns = out_weight.shape[1]
    f32, bf16 = jnp.float32, jnp.bfloat16
    vmem = pl.BlockSpec(memory_space=pltpu.VMEM)
    hbm = pl.BlockSpec(memory_space=pl.ANY)
    per = block_rows // LANES
    dma = pltpu.SemaphoreType.DMA
    forward, inverse = block_tables()
    return pl.pallas_call(
        block_kernel,
        out_shape=jax.ShapeDtypeStruct((block_rows, columns), f32),
        in_specs=[hbm] * 3 + [vmem] + [hbm] * 3,
        out_specs=hbm,
        scratch_shapes=[
            pltpu.VMEM((block_rows, width), f32),
            pltpu.VMEM((block_rows, width), f32),
            pltpu.VMEM((tap_rows, width), f32),
            pltpu.VMEM((block_rows, columns), f32),
            pltpu.VMEM((sources, narrow, block_rows), bf16),
            pltpu.VMEM((sources, narrow, tap_rows), bf16),
            pltpu.VMEM((seq_size, narrow, block_rows), bf16),
            pltpu.VMEM((sources, narrow, tap_rows), bf16),
            pltpu.VMEM((total // LANES, narrow, 2 * LANES), f32),
            pltpu.VMEM((total // LANES, narrow, 2 * LANES), f32),
            pltpu.VMEM((PAIR * per, narrow, 2 * LANES), f32),
            pltpu.VMEM((seq_size, narrow, block_rows), bf16),
            pltpu.VMEM((sources, narrow, block_rows), bf16),
            pltpu.VMEM((ch_size, halves, block_rows, half_width), bf16),
            pltpu.VMEM((ch_size, halves, half_width, columns), bf16),
            pltpu.VMEM(forward.shape, bf16),
            pltpu.VMEM(inverse.shape, bf16),
            dma((6,)),
            dma,
            dma((sources,)),
            dma((seq_size,)),
            dma((sources,)),
            dma((sources,)),
            dma((seq_size,)),
            dma((sources,)),
            dma((ch_size, halves)),
            dma((ch_size, halves)),
            pltpu.SemaphoreType.REGULAR((seq_size,)),
            pltpu.SemaphoreType.REGULAR((ch_size,)),
        ],
        compiler_params=pltpu.CompilerParams(
            collective_id=0, has_side_effects=True, vmem_limit_bytes=63000 * 1024
        ),
    )(
        values,
        gates,
        filter_taps,
        skip.reshape(1, width),
        out_weight.reshape(ch_size, halves, half_width, columns),
        jnp.asarray(forward),
        jnp.asarray(inverse),
    )


def local_body(values, gates, filter_taps, skip, out_weight):
    seq_size, ch_size = lax.axis_size("seq"), lax.axis_size("ch")
    block_rows, width = values.shape
    tap_rows = filter_taps.shape[0]
    total = block_rows * seq_size
    sources = min(tap_rows * seq_size, total) // tap_rows
    fits = (
        sources > 0
        and sources % PAIR == 0
        and seq_size % PAIR == 0
        and width % (sources * TILE) == 0
        and width // sources * PAIR % LANES == 0
        and ch_size % 2 == 0
        and block_rows % LANES == 0
        and tap_rows % block_rows == 0
        and total % tap_rows == 0
        and width // sources * total <= 256 * 1024
    )
    chosen = block_body if fits else body
    return chosen(values, gates, filter_taps, skip, out_weight)


def solution(mesh):
    placed = (P("seq", "ch"), P("seq", "ch"), P("seq", "ch"), P("ch"), P(None, "ch"))
    return jax.shard_map(
        local_body, mesh=mesh, in_specs=placed, out_specs=P("seq", "ch"), check_vma=False
    )
```

```python
import functools
import math

import jax
import jax.numpy as jnp
import numpy as np
from jax import lax
from jax.experimental import pallas as pl
from jax.experimental.pallas import tpu as pltpu
from jax.sharding import PartitionSpec as P

HIGHEST = lax.Precision.HIGHEST
MESH = pl.DeviceIdType.MESH
LANES = 128
TILE = 16
PAIR = 2


def split_length(length):
    leading = 1
    for factor in range(1, math.isqrt(length) + 1):
        if length % factor == 0:
            leading = factor
    return (leading, length // leading)


def phase_table(count_rows, count_cols, modulus):
    row_ids = jnp.arange(count_rows, dtype=jnp.int32)
    col_ids = jnp.arange(count_cols, dtype=jnp.int32)
    wrapped = row_ids[:, None] * col_ids[None, :] % modulus
    phases = 2.0 * math.pi / modulus * wrapped.astype(jnp.float32)
    return (jnp.cos(phases), jnp.sin(phases))


def complex_form(cosine, sine):
    upper = jnp.stack([cosine, -sine], axis=1)
    lower = jnp.stack([sine, cosine], axis=1)
    return jnp.stack([upper, lower], axis=0)


def transform_tables(length):
    rows_lead, rows_tail = split_length(length)
    cos_lead, sin_lead = phase_table(rows_lead, rows_lead, rows_lead)
    cos_tail, sin_tail = phase_table(rows_tail, rows_tail, rows_tail)
    cos_twist, sin_twist = phase_table(rows_lead, rows_tail, length)
    lead_table = jnp.stack([cos_lead, -sin_lead])
    tail_forward = complex_form(cos_tail, -sin_tail)
    tail_inverse = complex_form(cos_tail, sin_tail)
    return (
        lead_table,
        tail_forward,
        tail_inverse,
        cos_twist,
        sin_twist,
        rows_lead,
        rows_tail,
        length,
    )


def twist_rows(section, cosine, sine):
    real_part = section[0] * cosine[None] - section[1] * sine[None]
    imag_part = section[0] * sine[None] + section[1] * cosine[None]
    return jnp.stack([real_part, imag_part])


def forward_rows(rows, tables):
    lead_table, tail_forward, tail_inverse, cos_twist, sin_twist, rows_lead, rows_tail, length = (
        tables
    )
    signal = jnp.concatenate([rows, jnp.zeros_like(rows)], axis=1).reshape(
        rows.shape[0], rows_lead, rows_tail
    )
    section = jnp.einsum("pft,cts->pcfs", lead_table, signal, precision=HIGHEST)
    twisted = twist_rows(section, cos_twist, -sin_twist)
    return jnp.einsum("pgrs,rcfs->pcfg", tail_forward, twisted, precision=HIGHEST)


def inverse_rows(spectrum, tables):
    lead_table, tail_forward, tail_inverse, cos_twist, sin_twist, rows_lead, rows_tail, length = (
        tables
    )
    section = jnp.einsum("pgrs,rcfs->pcfg", tail_inverse, spectrum, precision=HIGHEST)
    twisted = twist_rows(section, cos_twist, sin_twist)
    signal = jnp.einsum("rft,rcfs->cts", lead_table, twisted, precision=HIGHEST) / length
    return signal.reshape(signal.shape[0], length)


def product(left, right):
    real_part = left[0] * right[0] - left[1] * right[1]
    imag_part = left[0] * right[1] + left[1] * right[0]
    return jnp.stack([real_part, imag_part])


def body(values, gates, filter_taps, skip, out_weight):
    block_rows, width = values.shape
    whole_filter = lax.all_gather(filter_taps, "seq", axis=0, tiled=True)
    devices = lax.axis_size("seq")
    narrow = width // devices
    whole_rows = lax.all_to_all(values.T, "seq", split_axis=0, concat_axis=1, tiled=True)
    total_rows = whole_rows.shape[1]
    own_taps = lax.dynamic_slice_in_dim(whole_filter, lax.axis_index("seq") * narrow, narrow, 1).T
    used_taps = min(own_taps.shape[1], total_rows)
    own_taps = own_taps[:, :used_taps]
    taps_rows = jnp.concatenate(
        [own_taps, jnp.zeros((narrow, total_rows - used_taps), jnp.float32)], axis=1
    )
    row_tables = transform_tables(2 * total_rows)
    spectrum = product(forward_rows(whole_rows, row_tables), forward_rows(taps_rows, row_tables))
    convolved_rows = inverse_rows(spectrum, row_tables)[:, :total_rows]
    convolved = lax.all_to_all(convolved_rows, "seq", split_axis=1, concat_axis=0, tiled=True).T
    hidden = (gates * (convolved + skip[None, :] * values)).astype(jnp.bfloat16)
    return jnp.dot(
        lax.all_gather(hidden, "ch", axis=1, tiled=True),
        out_weight,
        preferred_element_type=jnp.float32,
    )


def block_tables():
    size = 2 * LANES
    place = np.arange(size)[:, None]
    odd = 2 * np.arange(LANES)[None, :] + 1
    angle = np.pi / size * (place * odd % (2 * size))
    forward = np.concatenate([np.cos(angle), -np.sin(angle)], axis=1)
    inverse = forward[LANES:].T / LANES

    def two_parts(table, axis):
        high = table.astype(jnp.bfloat16)
        low = (table - high.astype(np.float64)).astype(jnp.bfloat16)
        return np.concatenate([high, low], axis=axis)

    return two_parts(forward, 0), two_parts(inverse, 1)


OUTS = 4


def block_kernel(
    values_hbm,
    gates_hbm,
    taps_hbm,
    skip_hbm,
    weight_hbm,
    tables_hbm,
    out_a,
    out_b,
    out_c,
    out_d,
    values_ref,
    gates_ref,
    taps_ref,
    skip_ref,
    x_out,
    h_out,
    x_in,
    h_in,
    x_tail,
    h_tail,
    x_waves,
    h_waves,
    y_waves,
    y_out,
    y_tail,
    y_in,
    hidden,
    weight,
    tables,
    load_sem,
    x_send,
    x_recv,
    h_send,
    h_recv,
    y_send,
    y_recv,
    g_send,
    g_recv,
    seq_ready,
    ch_ready,
):
    sources, narrow, block_rows = x_out.shape
    seq_size = x_in.shape[0]
    tap_rows = h_out.shape[2]
    ch_size, halves, _, half_width = hidden.shape
    per, pieces = block_rows // LANES, tap_rows // LANES
    hubs, keep = sources + PAIR, narrow - TILE
    early_taps = sources * block_rows // tap_rows
    me, lane_group = lax.axis_index("seq"), lax.axis_index("ch")
    f32, bf16 = jnp.float32, jnp.bfloat16

    loads = [
        pltpu.make_async_copy(source, target, load_sem.at[place])
        for place, (source, target) in enumerate(
            (
                (values_hbm, values_ref),
                (taps_hbm, taps_ref),
                (tables_hbm, tables),
                (gates_hbm, gates_ref),
                (skip_hbm, skip_ref),
                (weight_hbm, weight),
            )
        )
    ]
    for load in loads:
        load.start()

    barrier = pltpu.get_barrier_semaphore()
    for other in range(1, seq_size):
        @pl.when((me < other) & (me < hubs))
        def _():
            pl.semaphore_signal(barrier, inc=1, device_id={"seq": other}, device_id_type=MESH)
    for other in range(1, ch_size):
        @pl.when(lane_group < other)
        def _():
            pl.semaphore_signal(barrier, inc=1, device_id={"ch": other}, device_id_type=MESH)
    earlier = jnp.minimum(me, hubs) + lane_group

    @pl.when(earlier > 0)
    def _():
        pl.semaphore_wait(barrier, earlier)
    for other in range(hubs):
        @pl.when(me > other)
        def _():
            pl.semaphore_signal(
                seq_ready.at[me], inc=1, device_id={"seq": other}, device_id_type=MESH
            )
    for other in range(ch_size - 1):
        @pl.when(lane_group > other)
        def _():
            pl.semaphore_signal(
                ch_ready.at[lane_group], inc=1, device_id={"ch": other}, device_id_type=MESH
            )

    forward, inverse = tables.at[: 4 * LANES], tables.at[4 * LANES :]
    own, rest = pl.ds(0, keep), pl.ds(keep, TILE)

    def transfer(source, target, sends, recvs, to, place):
        return pltpu.make_async_remote_copy(
            source, target, sends.at[to], recvs.at[place],
            device_id={"seq": to}, device_id_type=MESH,
        )

    def tails_of(helper):
        return pl.ds((helper - sources) * PAIR, PAIR)

    def x_copy(to, place, late):
        if to >= sources:
            source, target = x_out.at[tails_of(to), rest], x_tail.at[place]
        elif late:
            source, target = x_out.at[to, own], x_in.at[place, own]
        else:
            source, target = x_out.at[to], x_in.at[place]
        return transfer(source, target, x_send, x_recv, to, place)

    def h_copy(to, place, late):
        if to >= sources:
            source, target = h_out.at[tails_of(to), rest], h_tail.at[place]
        elif late:
            source, target = h_out.at[to, own], h_in.at[place, own]
        else:
            source, target = h_out.at[to], h_in.at[place]
        return transfer(source, target, h_send, h_recv, to, place)

    def y_copy(to, place):
        if to >= sources:
            source, target = y_out.at[to, own], y_in.at[place, own]
        else:
            source, target = y_out.at[to], y_in.at[place]
        return transfer(source, target, y_send, y_recv, to, place)

    def tail_copy(to, helper, place):
        target = y_in.at[pl.ds((helper - sources) * PAIR, PAIR), rest]
        return transfer(y_tail.at[to], target, y_send, y_recv, to, place)

    def ready(to):
        @pl.when(me < to)
        def _():
            pl.semaphore_wait(seq_ready.at[to], 1)

    loads[0].wait()
    x_out[...] = values_ref[...].T.astype(bf16).reshape(x_out.shape)

    @pl.when(me >= sources)
    def _():
        for to in range(hubs):
            if to >= sources:
                ready(to)

            @pl.when(me != to)
            def _():
                x_copy(to, me, True).start()

    loads[1].wait()

    @pl.when(me < sources)
    def _():
        h_out[...] = taps_ref[...].T.astype(bf16).reshape(h_out.shape)
        for to in range(hubs):
            ready(to)

            @pl.when(me != to)
            def _():
                x_copy(to, me, False).start()

            @pl.when((me != to) & (me < early_taps))
            def _():
                h_copy(to, me, False).start()

            @pl.when((me != to) & (me >= early_taps))
            def _():
                h_copy(to, me, True).start()
        x_in[me] = x_out[me]
        h_in[me] = h_out[me]

    loads[2].wait()

    def take_taps(source, helper):
        late = source >= early_taps
        if helper:
            h_copy(sources, source, late).wait_recv()
            taps, count = h_tail.at[source], PAIR * TILE
        else:
            @pl.when(me != source)
            def _():
                h_copy(0, source, late).wait_recv()

            taps, count = h_in.at[source], keep if late else narrow
        rows = []
        for piece in range(pieces):
            lanes = slice(piece * LANES, (piece + 1) * LANES)
            block = taps[:, :, lanes].reshape(count, LANES) if helper else taps[:count, lanes]
            rows.append(jnp.concatenate([block, block], axis=1))
        table = jnp.concatenate([forward[:LANES], forward[2 * LANES : 3 * LANES]], axis=0)
        waves = jnp.dot(jnp.concatenate(rows, axis=0), table, preferred_element_type=f32)
        h_waves[source * pieces : (source + 1) * pieces, :count] = waves.reshape(
            pieces, count, 2 * LANES
        )

    def take_values(first, helper):
        late = first >= sources
        count = PAIR * TILE if helper else keep if late else narrow
        for source in range(first, first + PAIR):
            @pl.when(me != source)
            def _():
                x_copy(sources if helper else 0, source, late).wait_recv()

        def piece_of(source, piece):
            lanes = slice(piece * LANES, (piece + 1) * LANES)
            if helper:
                return x_tail[source, :, :, lanes].reshape(count, LANES)
            return x_in[source, :count, lanes]

        before = piece_of(first - 1, per - 1) if first else jnp.zeros((count, LANES), bf16)
        rows = []
        for source in range(first, first + PAIR):
            for piece in range(per):
                here = piece_of(source, piece)
                rows.append(jnp.concatenate([before, here, before, here], axis=1))
                before = here
        waves = jnp.dot(
            jnp.concatenate(rows, axis=0), forward[...], preferred_element_type=f32
        )
        x_waves[first * per : (first + PAIR) * per, :count] = waves.reshape(
            PAIR * per, count, 2 * LANES
        )

    def multiply(first, low, high, fresh, tiles):
        start, count = first * per, PAIR * per

        def one(part, carry):
            rows = pl.ds(pl.multiple_of(part * TILE, TILE), TILE)
            real_lanes, imag_lanes = slice(0, LANES), slice(LANES, 2 * LANES)
            cache = {}

            def x_part(block):
                if block not in cache:
                    cache[block] = (
                        x_waves[block, rows, real_lanes], x_waves[block, rows, imag_lanes]
                    )
                return cache[block]

            sums = [None] * count
            if not fresh:
                sums = [
                    (y_waves[start + spot, rows, real_lanes], y_waves[start + spot, rows, imag_lanes])
                    for spot in range(count)
                ]
            for lag in range(max(0, start - high + 1), start + count - low):
                h_real, h_imag = h_waves[lag, rows, real_lanes], h_waves[lag, rows, imag_lanes]
                for spot in range(count):
                    block = start + spot - lag
                    if not low <= block < high:
                        continue
                    x_real, x_imag = x_part(block)
                    real = x_real * h_real - x_imag * h_imag
                    imag = x_real * h_imag + x_imag * h_real
                    if sums[spot] is not None:
                        real, imag = sums[spot][0] + real, sums[spot][1] + imag
                    sums[spot] = (real, imag)
            for spot in range(count):
                y_waves[start + spot, rows, real_lanes] = sums[spot][0]
                y_waves[start + spot, rows, imag_lanes] = sums[spot][1]
            return carry

        lax.fori_loop(0, tiles, one, 0)

    def give_back(first, helper):
        count = PAIR * TILE if helper else keep if first >= sources else narrow
        waves = y_waves[first * per : (first + PAIR) * per, :count].reshape(
            PAIR * per * count, 2 * LANES
        )
        high = waves.astype(bf16)
        low = (waves - high.astype(f32)).astype(bf16)
        both = jnp.dot(high, inverse[...], preferred_element_type=f32)
        more = jnp.dot(low, inverse[:, :LANES], preferred_element_type=f32)
        convolved = (both[:, :LANES] + both[:, LANES:] + more).astype(bf16)
        for spot in range(PAIR * per):
            to, piece = first + spot // per, spot % per
            lanes = slice(piece * LANES, (piece + 1) * LANES)
            part = convolved[spot * count : (spot + 1) * count]
            if helper:
                y_tail[to, :, :, lanes] = part.reshape(PAIR, TILE, LANES)
            else:
                y_out[to, :count, lanes] = part
        for to in range(first, first + PAIR):
            if to >= hubs:
                pl.semaphore_wait(seq_ready.at[to], 1)
            if not helper:
                @pl.when(me != to)
                def _():
                    y_copy(to, me).start()
            else:
                for which in range(sources, hubs):
                    @pl.when((me == which) & (me != to))
                    def _():
                        tail_copy(to, which, me).start()

    def convolve(helper):
        tiles = PAIR if helper else narrow // TILE
        for source in range(sources):
            if source < early_taps:
                take_taps(source, helper)
        for first in range(0, sources, PAIR):
            take_values(first, helper)
            if not helper:
                multiply(first, 0, (first + PAIR) * per, True, tiles)
                give_back(first, helper)
        if not helper:
            tiles = keep // TILE
        for source in range(early_taps, sources):
            take_taps(source, helper)
        for first in range(sources, seq_size, PAIR):
            multiply(first, 0, sources * per, True, tiles)
        for fresh in range(sources, seq_size, PAIR):
            take_values(fresh, helper)
            multiply(fresh, fresh * per, (fresh + PAIR) * per, False, tiles)
            give_back(fresh, helper)
            for first in range(fresh + PAIR, seq_size, PAIR):
                multiply(first, fresh * per, (fresh + PAIR) * per, False, tiles)

    @pl.when(me < sources)
    def _():
        convolve(False)
        y_in[me] = y_out[me]

    for which in range(sources, hubs):
        @pl.when(me == which)
        def _():
            tails = slice((which - sources) * PAIR, (which - sources + 1) * PAIR)
            x_tail[which] = x_out[tails, keep:]

    @pl.when((me >= sources) & (me < hubs))
    def _():
        convolve(True)

    for which in range(sources, hubs):
        @pl.when(me == which)
        def _():
            tails = slice((which - sources) * PAIR, (which - sources + 1) * PAIR)
            y_in[tails, keep:] = y_tail[which]

    partner = lane_group + 1 - 2 * lax.rem(lane_group, 2)
    pairs = ch_size // 2
    lead = jnp.minimum(me // PAIR, halves - 1)
    order = [lax.rem(lead + turn, halves) for turn in range(halves)]

    def spread(kind, half, slot, to):
        block = hidden.at[slot, half]
        copy = pltpu.make_async_remote_copy(
            block, block, g_send.at[kind, half], g_recv.at[kind, half],
            device_id={"ch": to}, device_id_type=MESH,
        )
        copy.start()
        g_copies.append(copy)
        return copy

    def add_product(half, slot, first=False):
        term = jnp.dot(hidden[slot, half], weight[slot, half], preferred_element_type=f32)
        for place, out in enumerate(outs):
            part = term[place * out_rows : (place + 1) * out_rows]
            out[...] = part if first else out[...] + part

    for other in range(1, ch_size):
        @pl.when(lane_group < other)
        def _():
            pl.semaphore_wait(ch_ready.at[other], 1)

    outs = (out_a, out_b, out_c, out_d)
    out_rows = out_a.shape[0]
    g_copies, direct, relayed = [], {}, {}
    for load in loads[3:5]:
        load.wait()
    for turn, half in enumerate(order):
        for part in range(PAIR):
            source = half * PAIR + part

            @pl.when((me != source) & (me < sources))
            def _():
                y_copy(0, source).wait_recv()

            @pl.when(me >= sources)
            def _():
                y_copy(sources, source).wait_recv()

        @pl.when((me >= sources) & (me != sources + half))
        def _():
            tail_copy(sources, sources, sources + half).wait_recv()
        convolved = y_in[pl.ds(half * PAIR, PAIR)].astype(f32).reshape(half_width, block_rows).T
        span = pl.ds(pl.multiple_of(half * half_width, half_width), half_width)
        hidden[lane_group, half] = (
            gates_ref[:, span] * (convolved + skip_ref[:, span] * values_ref[:, span])
        ).astype(bf16)
        for pair in range(1, pairs):
            direct[pair, turn] = spread(
                2 * pair - 1, half, lane_group, lax.rem(lane_group + 2 * pair, ch_size)
            )
        direct[0, turn] = spread(0, half, lane_group, partner)
    loads[5].wait()
    for turn, half in enumerate(order):
        add_product(half, lane_group, not turn)
    for turn, half in enumerate(order):
        direct[0, turn].wait_recv()
        add_product(half, partner)
        for pair in range(1, pairs):
            slot = lax.rem(lane_group + ch_size - 2 * pair, ch_size)
            direct[pair, turn].wait_recv()
            relayed[pair, turn] = spread(2 * pair, half, slot, partner)
            add_product(half, slot)
    for turn, half in enumerate(order):
        for pair in range(1, pairs):
            slot = lax.rem(partner + ch_size - 2 * pair, ch_size)
            relayed[pair, turn].wait_recv()
            add_product(half, slot)

    for copy in g_copies:
        copy.wait_send()
    for to in range(hubs):
        for late in (False, True):
            @pl.when((me != to) & ((me >= sources) == late))
            def _():
                x_copy(to, me, late).wait_send()

            @pl.when((me != to) & (me < sources) & ((me >= early_taps) == late))
            def _():
                h_copy(to, me, late).wait_send()
    for to in range(seq_size):
        @pl.when((me != to) & (me < sources))
        def _():
            y_copy(to, me).wait_send()

        if to >= sources:
            @pl.when((me != to) & (me >= sources) & (me < hubs))
            def _():
                tail_copy(to, sources, me).wait_send()


def block_body(values, gates, filter_taps, skip, out_weight):
    seq_size, ch_size = lax.axis_size("seq"), lax.axis_size("ch")
    block_rows, width = values.shape
    tap_rows = filter_taps.shape[0]
    total = block_rows * seq_size
    sources = min(tap_rows * seq_size, total) // tap_rows
    narrow, halves, hubs = width // sources, sources // PAIR, sources + PAIR
    half_width = width // halves
    columns = out_weight.shape[1]
    f32, bf16 = jnp.float32, jnp.bfloat16
    hbm = pl.BlockSpec(memory_space=pl.ANY)
    dma = pltpu.SemaphoreType.DMA
    tables = np.concatenate(block_tables(), axis=0)
    outs = pl.pallas_call(
        block_kernel,
        out_shape=[jax.ShapeDtypeStruct((block_rows // OUTS, columns), f32)] * OUTS,
        in_specs=[hbm] * 6,
        out_specs=[pl.BlockSpec(memory_space=pltpu.VMEM)] * OUTS,
        scratch_shapes=[
            pltpu.VMEM((block_rows, width), f32),
            pltpu.VMEM((block_rows, width), f32),
            pltpu.VMEM((tap_rows, width), f32),
            pltpu.VMEM((1, width), f32),
            pltpu.VMEM((sources, narrow, block_rows), bf16),
            pltpu.VMEM((sources, narrow, tap_rows), bf16),
            pltpu.VMEM((seq_size, narrow, block_rows), bf16),
            pltpu.VMEM((sources, narrow, tap_rows), bf16),
            pltpu.VMEM((seq_size, PAIR, TILE, block_rows), bf16),
            pltpu.VMEM((sources, PAIR, TILE, tap_rows), bf16),
            pltpu.VMEM((total // LANES, narrow, 2 * LANES), f32),
            pltpu.VMEM((total // LANES, narrow, 2 * LANES), f32),
            pltpu.VMEM((total // LANES, narrow, 2 * LANES), f32),
            pltpu.VMEM((seq_size, narrow, block_rows), bf16),
            pltpu.VMEM((seq_size, PAIR, TILE, block_rows), bf16),
            pltpu.VMEM((sources, narrow, block_rows), bf16),
            pltpu.VMEM((ch_size, halves, block_rows, half_width), bf16),
            pltpu.VMEM((ch_size, halves, half_width, columns), bf16),
            pltpu.VMEM(tables.shape, bf16),
            dma((6,)),
            dma((hubs,)),
            dma((seq_size,)),
            dma((hubs,)),
            dma((sources,)),
            dma((seq_size,)),
            dma((hubs,)),
            dma((ch_size, halves)),
            dma((ch_size, halves)),
            pltpu.SemaphoreType.REGULAR((seq_size,)),
            pltpu.SemaphoreType.REGULAR((ch_size,)),
        ],
        compiler_params=pltpu.CompilerParams(
            collective_id=0, has_side_effects=True, vmem_limit_bytes=54500*1024
        ),
    )(
        values,
        gates,
        filter_taps,
        skip.reshape(1, width),
        out_weight.reshape(ch_size, halves, half_width, columns),
        jnp.asarray(tables),
    )
    return jnp.concatenate(outs, axis=0)


def local_body(values, gates, filter_taps, skip, out_weight):
    seq_size, ch_size = lax.axis_size("seq"), lax.axis_size("ch")
    block_rows, width = values.shape
    tap_rows = filter_taps.shape[0]
    total = block_rows * seq_size
    sources = min(tap_rows * seq_size, total) // tap_rows
    fits = (
        sources == PAIR * PAIR
        and seq_size % PAIR == 0
        and seq_size >= sources + PAIR
        and width % (sources * TILE) == 0
        and width // sources > TILE
        and width // sources * PAIR % LANES == 0
        and ch_size % 2 == 0
        and block_rows % LANES == 0
        and tap_rows % block_rows == 0
        and sources * block_rows % tap_rows == 0
        and total % tap_rows == 0
        and width // sources * total <= 256 * 1024
    )
    chosen = block_body if fits else body
    return chosen(values, gates, filter_taps, skip, out_weight)


def solution(mesh):
    placed = (P("seq", "ch"), P("seq", "ch"), P("seq", "ch"), P("ch"), P(None, "ch"))
    return jax.shard_map(
        local_body, mesh=mesh, in_specs=placed, out_specs=P("seq", "ch"), check_vma=False
    )
```

```python
import functools
import math

import jax
import jax.numpy as jnp
import numpy as np
from jax import lax
from jax.experimental import pallas as pl
from jax.experimental.pallas import tpu as pltpu
from jax.sharding import PartitionSpec as P

HIGHEST = lax.Precision.HIGHEST
MESH = pl.DeviceIdType.MESH
LANES = 128
TILE = 16
PAIR = 2


def split_length(length):
    leading = 1
    for factor in range(1, math.isqrt(length) + 1):
        if length % factor == 0:
            leading = factor
    return (leading, length // leading)


def phase_table(count_rows, count_cols, modulus):
    row_ids = jnp.arange(count_rows, dtype=jnp.int32)
    col_ids = jnp.arange(count_cols, dtype=jnp.int32)
    wrapped = row_ids[:, None] * col_ids[None, :] % modulus
    phases = 2.0 * math.pi / modulus * wrapped.astype(jnp.float32)
    return (jnp.cos(phases), jnp.sin(phases))


def complex_form(cosine, sine):
    upper = jnp.stack([cosine, -sine], axis=1)
    lower = jnp.stack([sine, cosine], axis=1)
    return jnp.stack([upper, lower], axis=0)


def transform_tables(length):
    rows_lead, rows_tail = split_length(length)
    cos_lead, sin_lead = phase_table(rows_lead, rows_lead, rows_lead)
    cos_tail, sin_tail = phase_table(rows_tail, rows_tail, rows_tail)
    cos_twist, sin_twist = phase_table(rows_lead, rows_tail, length)
    lead_table = jnp.stack([cos_lead, -sin_lead])
    tail_forward = complex_form(cos_tail, -sin_tail)
    tail_inverse = complex_form(cos_tail, sin_tail)
    return (
        lead_table,
        tail_forward,
        tail_inverse,
        cos_twist,
        sin_twist,
        rows_lead,
        rows_tail,
        length,
    )


def twist_rows(section, cosine, sine):
    real_part = section[0] * cosine[None] - section[1] * sine[None]
    imag_part = section[0] * sine[None] + section[1] * cosine[None]
    return jnp.stack([real_part, imag_part])


def forward_rows(rows, tables):
    lead_table, tail_forward, tail_inverse, cos_twist, sin_twist, rows_lead, rows_tail, length = (
        tables
    )
    signal = jnp.concatenate([rows, jnp.zeros_like(rows)], axis=1).reshape(
        rows.shape[0], rows_lead, rows_tail
    )
    section = jnp.einsum("pft,cts->pcfs", lead_table, signal, precision=HIGHEST)
    twisted = twist_rows(section, cos_twist, -sin_twist)
    return jnp.einsum("pgrs,rcfs->pcfg", tail_forward, twisted, precision=HIGHEST)


def inverse_rows(spectrum, tables):
    lead_table, tail_forward, tail_inverse, cos_twist, sin_twist, rows_lead, rows_tail, length = (
        tables
    )
    section = jnp.einsum("pgrs,rcfs->pcfg", tail_inverse, spectrum, precision=HIGHEST)
    twisted = twist_rows(section, cos_twist, sin_twist)
    signal = jnp.einsum("rft,rcfs->cts", lead_table, twisted, precision=HIGHEST) / length
    return signal.reshape(signal.shape[0], length)


def product(left, right):
    real_part = left[0] * right[0] - left[1] * right[1]
    imag_part = left[0] * right[1] + left[1] * right[0]
    return jnp.stack([real_part, imag_part])


def body(values, gates, filter_taps, skip, out_weight):
    block_rows, width = values.shape
    whole_filter = lax.all_gather(filter_taps, "seq", axis=0, tiled=True)
    devices = lax.axis_size("seq")
    narrow = width // devices
    whole_rows = lax.all_to_all(values.T, "seq", split_axis=0, concat_axis=1, tiled=True)
    total_rows = whole_rows.shape[1]
    own_taps = lax.dynamic_slice_in_dim(whole_filter, lax.axis_index("seq") * narrow, narrow, 1).T
    used_taps = min(own_taps.shape[1], total_rows)
    own_taps = own_taps[:, :used_taps]
    taps_rows = jnp.concatenate(
        [own_taps, jnp.zeros((narrow, total_rows - used_taps), jnp.float32)], axis=1
    )
    row_tables = transform_tables(2 * total_rows)
    spectrum = product(forward_rows(whole_rows, row_tables), forward_rows(taps_rows, row_tables))
    convolved_rows = inverse_rows(spectrum, row_tables)[:, :total_rows]
    convolved = lax.all_to_all(convolved_rows, "seq", split_axis=1, concat_axis=0, tiled=True).T
    hidden = (gates * (convolved + skip[None, :] * values)).astype(jnp.bfloat16)
    return jnp.dot(
        lax.all_gather(hidden, "ch", axis=1, tiled=True),
        out_weight,
        preferred_element_type=jnp.float32,
    )


def block_tables():
    size = 2 * LANES
    place = np.arange(size)[:, None]
    odd = 2 * np.arange(LANES)[None, :] + 1
    angle = np.pi / size * (place * odd % (2 * size))
    forward = np.concatenate([np.cos(angle), -np.sin(angle)], axis=1)
    inverse = forward[LANES:].T / LANES

    def two_parts(table, axis):
        high = table.astype(jnp.bfloat16)
        low = (table - high.astype(np.float64)).astype(jnp.bfloat16)
        return np.concatenate([high, low], axis=axis)

    return two_parts(forward, 0), two_parts(inverse, 1)


OUTS = 4


def block_kernel(
    values_hbm,
    gates_hbm,
    taps_hbm,
    skip_hbm,
    weight_hbm,
    tables_hbm,
    out_a,
    out_b,
    out_c,
    out_d,
    values_ref,
    gates_ref,
    taps_ref,
    skip_ref,
    x_out,
    h_out,
    x_in,
    h_in,
    x_tail,
    h_tail,
    x_waves,
    h_waves,
    y_waves,
    y_out,
    y_tail,
    y_in,
    hidden,
    weight,
    tables,
    load_sem,
    x_send,
    x_recv,
    h_send,
    h_recv,
    y_send,
    y_recv,
    g_send,
    g_recv,
    seq_ready,
    ch_ready,
):
    sources, narrow, block_rows = x_out.shape
    seq_size = x_in.shape[0]
    tap_rows = h_out.shape[2]
    ch_size, halves, _, half_width = hidden.shape
    per, pieces = block_rows // LANES, tap_rows // LANES
    hubs, keep = sources + PAIR, narrow - TILE
    early_taps = sources * block_rows // tap_rows
    me, lane_group = lax.axis_index("seq"), lax.axis_index("ch")
    f32, bf16 = jnp.float32, jnp.bfloat16

    loads = [
        pltpu.make_async_copy(source, target, load_sem.at[place])
        for place, (source, target) in enumerate(
            (
                (values_hbm, values_ref),
                (taps_hbm, taps_ref),
                (tables_hbm, tables),
                (gates_hbm, gates_ref),
                (skip_hbm, skip_ref),
                (weight_hbm, weight),
            )
        )
    ]
    for load in loads:
        load.start()

    barrier = pltpu.get_barrier_semaphore()
    for other in range(1, seq_size):
        @pl.when((me < other) & (me < hubs))
        def _():
            pl.semaphore_signal(barrier, inc=1, device_id={"seq": other}, device_id_type=MESH)
    for other in range(1, ch_size):
        @pl.when(lane_group < other)
        def _():
            pl.semaphore_signal(barrier, inc=1, device_id={"ch": other}, device_id_type=MESH)
    earlier = jnp.minimum(me, hubs) + lane_group

    @pl.when(earlier > 0)
    def _():
        pl.semaphore_wait(barrier, earlier)
    for other in range(hubs):
        @pl.when(me > other)
        def _():
            pl.semaphore_signal(
                seq_ready.at[me], inc=1, device_id={"seq": other}, device_id_type=MESH
            )
    for other in range(ch_size - 1):
        @pl.when(lane_group > other)
        def _():
            pl.semaphore_signal(
                ch_ready.at[lane_group], inc=1, device_id={"ch": other}, device_id_type=MESH
            )

    forward, inverse = tables.at[: 4 * LANES], tables.at[4 * LANES :]
    own, rest = pl.ds(0, keep), pl.ds(keep, TILE)

    def transfer(source, target, sends, recvs, to, place):
        return pltpu.make_async_remote_copy(
            source, target, sends.at[to], recvs.at[place],
            device_id={"seq": to}, device_id_type=MESH,
        )

    def tails_of(helper):
        return pl.ds((helper - sources) * PAIR, PAIR)

    def x_copy(to, place, late):
        if to >= sources:
            source, target = x_out.at[tails_of(to), rest], x_tail.at[place]
        elif late:
            source, target = x_out.at[to, own], x_in.at[place, own]
        else:
            source, target = x_out.at[to], x_in.at[place]
        return transfer(source, target, x_send, x_recv, to, place)

    def h_copy(to, place, late):
        if to >= sources:
            source, target = h_out.at[tails_of(to), rest], h_tail.at[place]
        elif late:
            source, target = h_out.at[to, own], h_in.at[place, own]
        else:
            source, target = h_out.at[to], h_in.at[place]
        return transfer(source, target, h_send, h_recv, to, place)

    def y_copy(to, place):
        if to >= sources:
            source, target = y_out.at[to, own], y_in.at[place, own]
        else:
            source, target = y_out.at[to], y_in.at[place]
        return transfer(source, target, y_send, y_recv, to, place)

    def tail_copy(to, helper, place):
        target = y_in.at[pl.ds((helper - sources) * PAIR, PAIR), rest]
        return transfer(y_tail.at[to], target, y_send, y_recv, to, place)

    def ready(to):
        @pl.when(me < to)
        def _():
            pl.semaphore_wait(seq_ready.at[to], 1)

    loads[0].wait()
    x_out[...] = values_ref[...].T.astype(bf16).reshape(x_out.shape)

    @pl.when(me >= sources)
    def _():
        for to in range(hubs):
            if to >= sources:
                ready(to)

            @pl.when(me != to)
            def _():
                x_copy(to, me, True).start()

    loads[1].wait()

    @pl.when(me < sources)
    def _():
        h_out[...] = taps_ref[...].T.astype(bf16).reshape(h_out.shape)
        for to in range(hubs):
            ready(to)

            @pl.when(me != to)
            def _():
                x_copy(to, me, False).start()

            @pl.when((me != to) & (me < early_taps))
            def _():
                h_copy(to, me, False).start()

            @pl.when((me != to) & (me >= early_taps))
            def _():
                h_copy(to, me, True).start()
        x_in[me] = x_out[me]
        h_in[me] = h_out[me]

    loads[2].wait()

    def take_taps(source, helper):
        late = source >= early_taps
        if helper:
            h_copy(sources, source, late).wait_recv()
            taps, count = h_tail.at[source], PAIR * TILE
        else:
            @pl.when(me != source)
            def _():
                h_copy(0, source, late).wait_recv()

            taps, count = h_in.at[source], keep if late else narrow
        rows = []
        for piece in range(pieces):
            lanes = slice(piece * LANES, (piece + 1) * LANES)
            block = taps[:, :, lanes].reshape(count, LANES) if helper else taps[:count, lanes]
            rows.append(jnp.concatenate([block, block], axis=1))
        table = jnp.concatenate([forward[:LANES], forward[2 * LANES : 3 * LANES]], axis=0)
        waves = jnp.dot(jnp.concatenate(rows, axis=0), table, preferred_element_type=f32)
        h_waves[source * pieces : (source + 1) * pieces, :count] = waves.reshape(
            pieces, count, 2 * LANES
        )

    def take_values(first, helper):
        late = first >= sources
        count = PAIR * TILE if helper else keep if late else narrow
        for source in range(first, first + PAIR):
            @pl.when(me != source)
            def _():
                x_copy(sources if helper else 0, source, late).wait_recv()

        def piece_of(source, piece):
            lanes = slice(piece * LANES, (piece + 1) * LANES)
            if helper:
                return x_tail[source, :, :, lanes].reshape(count, LANES)
            return x_in[source, :count, lanes]

        before = piece_of(first - 1, per - 1) if first else jnp.zeros((count, LANES), bf16)
        rows = []
        for source in range(first, first + PAIR):
            for piece in range(per):
                here = piece_of(source, piece)
                rows.append(jnp.concatenate([before, here, before, here], axis=1))
                before = here
        waves = jnp.dot(
            jnp.concatenate(rows, axis=0), forward[...], preferred_element_type=f32
        )
        x_waves[first * per : (first + PAIR) * per, :count] = waves.reshape(
            PAIR * per, count, 2 * LANES
        )

    def multiply(first, low, high, fresh, tiles):
        start, count = first * per, PAIR * per

        def one(part, carry):
            rows = pl.ds(pl.multiple_of(part * TILE, TILE), TILE)
            real_lanes, imag_lanes = slice(0, LANES), slice(LANES, 2 * LANES)
            cache = {}

            def x_part(block):
                if block not in cache:
                    cache[block] = (
                        x_waves[block, rows, real_lanes], x_waves[block, rows, imag_lanes]
                    )
                return cache[block]

            sums = [None] * count
            if not fresh:
                sums = [
                    (y_waves[start + spot, rows, real_lanes], y_waves[start + spot, rows, imag_lanes])
                    for spot in range(count)
                ]
            for lag in range(max(0, start - high + 1), start + count - low):
                h_real, h_imag = h_waves[lag, rows, real_lanes], h_waves[lag, rows, imag_lanes]
                for spot in range(count):
                    block = start + spot - lag
                    if not low <= block < high:
                        continue
                    x_real, x_imag = x_part(block)
                    real = x_real * h_real - x_imag * h_imag
                    imag = x_real * h_imag + x_imag * h_real
                    if sums[spot] is not None:
                        real, imag = sums[spot][0] + real, sums[spot][1] + imag
                    sums[spot] = (real, imag)
            for spot in range(count):
                y_waves[start + spot, rows, real_lanes] = sums[spot][0]
                y_waves[start + spot, rows, imag_lanes] = sums[spot][1]
            return carry

        lax.fori_loop(0, tiles, one, 0)

    def give_back(first, helper):
        count = PAIR * TILE if helper else keep if first >= sources else narrow
        waves = y_waves[first * per : (first + PAIR) * per, :count].reshape(
            PAIR * per * count, 2 * LANES
        )
        high = waves.astype(bf16)
        low = (waves - high.astype(f32)).astype(bf16)
        both = jnp.dot(high, inverse[...], preferred_element_type=f32)
        more = jnp.dot(low, inverse[:, :LANES], preferred_element_type=f32)
        convolved = (both[:, :LANES] + both[:, LANES:] + more).astype(bf16)
        for spot in range(PAIR * per):
            to, piece = first + spot // per, spot % per
            lanes = slice(piece * LANES, (piece + 1) * LANES)
            part = convolved[spot * count : (spot + 1) * count]
            if helper:
                y_tail[to, :, :, lanes] = part.reshape(PAIR, TILE, LANES)
            else:
                y_out[to, :count, lanes] = part
        for to in range(first, first + PAIR):
            if to >= hubs:
                pl.semaphore_wait(seq_ready.at[to], 1)
            if not helper:
                @pl.when(me != to)
                def _():
                    y_copy(to, me).start()
            else:
                for which in range(sources, hubs):
                    @pl.when((me == which) & (me != to))
                    def _():
                        tail_copy(to, which, me).start()

    def convolve(helper):
        tiles = PAIR if helper else narrow // TILE
        for source in range(sources):
            if source < early_taps:
                take_taps(source, helper)
        for first in range(0, sources, PAIR):
            take_values(first, helper)
            if not helper:
                multiply(first, 0, (first + PAIR) * per, True, tiles)
                give_back(first, helper)
        if not helper:
            tiles = keep // TILE
        for source in range(early_taps, sources):
            take_taps(source, helper)
        for first in range(sources, seq_size, PAIR):
            multiply(first, 0, sources * per, True, tiles)
        for fresh in range(sources, seq_size, PAIR):
            take_values(fresh, helper)
            multiply(fresh, fresh * per, (fresh + PAIR) * per, False, tiles)
            give_back(fresh, helper)
            for first in range(fresh + PAIR, seq_size, PAIR):
                multiply(first, fresh * per, (fresh + PAIR) * per, False, tiles)

    @pl.when(me < sources)
    def _():
        convolve(False)
        y_in[me] = y_out[me]

    for which in range(sources, hubs):
        @pl.when(me == which)
        def _():
            tails = slice((which - sources) * PAIR, (which - sources + 1) * PAIR)
            x_tail[which] = x_out[tails, keep:]

    @pl.when((me >= sources) & (me < hubs))
    def _():
        convolve(True)

    for which in range(sources, hubs):
        @pl.when(me == which)
        def _():
            tails = slice((which - sources) * PAIR, (which - sources + 1) * PAIR)
            y_in[tails, keep:] = y_tail[which]

    partner = lane_group + 1 - 2 * lax.rem(lane_group, 2)
    pairs = ch_size // 2

    def spread(kind, half, slot, to):
        block = hidden.at[slot, half]
        copy = pltpu.make_async_remote_copy(
            block, block, g_send.at[kind, half], g_recv.at[kind, half],
            device_id={"ch": to}, device_id_type=MESH,
        )
        copy.start()
        g_copies.append(copy)
        return copy

    def add_product(half, slot, first=False):
        term = jnp.dot(hidden[slot, half], weight[slot, half], preferred_element_type=f32)
        for place, out in enumerate(outs):
            part = term[place * out_rows : (place + 1) * out_rows]
            out[...] = part if first else out[...] + part

    for other in range(1, ch_size):
        @pl.when(lane_group < other)
        def _():
            pl.semaphore_wait(ch_ready.at[other], 1)

    outs = (out_a, out_b, out_c, out_d)
    out_rows = out_a.shape[0]
    g_copies, direct, relayed = [], {}, {}
    for load in loads[3:5]:
        load.wait()
    for half in range(halves):
        for part in range(PAIR):
            source = half * PAIR + part

            @pl.when((me != source) & (me < sources))
            def _():
                y_copy(0, source).wait_recv()

            @pl.when(me >= sources)
            def _():
                y_copy(sources, source).wait_recv()

        @pl.when((me >= sources) & (me != sources + half))
        def _():
            tail_copy(sources, sources, sources + half).wait_recv()
        convolved = y_in[half * PAIR : (half + 1) * PAIR].astype(f32).reshape(half_width, block_rows).T
        span = slice(half * half_width, (half + 1) * half_width)
        hidden[lane_group, half] = (
            gates_ref[:, span] * (convolved + skip_ref[:, span] * values_ref[:, span])
        ).astype(bf16)
        for pair in range(1, pairs):
            direct[pair, half] = spread(
                2 * pair - 1, half, lane_group, lax.rem(lane_group + 2 * pair, ch_size)
            )
            if half == halves - 1:
                relayed[pair, half] = spread(
                    2 * pair, half, lane_group, lax.rem(partner + 2 * pair, ch_size)
                )
        direct[0, half] = spread(0, half, lane_group, partner)
    loads[5].wait()
    for half in range(halves):
        add_product(half, lane_group, not half)
    for half in range(halves):
        direct[0, half].wait_recv()
        add_product(half, partner)
        for pair in range(1, pairs):
            slot = lax.rem(lane_group + ch_size - 2 * pair, ch_size)
            direct[pair, half].wait_recv()
            if half < halves - 1:
                relayed[pair, half] = spread(2 * pair, half, slot, partner)
            add_product(half, slot)
    for half in range(halves):
        for pair in range(1, pairs):
            slot = lax.rem(partner + ch_size - 2 * pair, ch_size)
            relayed[pair, half].wait_recv()
            add_product(half, slot)

    for copy in g_copies:
        copy.wait_send()
    for to in range(hubs):
        for late in (False, True):
            @pl.when((me != to) & ((me >= sources) == late))
            def _():
                x_copy(to, me, late).wait_send()

            @pl.when((me != to) & (me < sources) & ((me >= early_taps) == late))
            def _():
                h_copy(to, me, late).wait_send()
    for to in range(seq_size):
        @pl.when((me != to) & (me < sources))
        def _():
            y_copy(to, me).wait_send()

        if to >= sources:
            @pl.when((me != to) & (me >= sources) & (me < hubs))
            def _():
                tail_copy(to, sources, me).wait_send()


def block_body(values, gates, filter_taps, skip, out_weight):
    seq_size, ch_size = lax.axis_size("seq"), lax.axis_size("ch")
    block_rows, width = values.shape
    tap_rows = filter_taps.shape[0]
    total = block_rows * seq_size
    sources = min(tap_rows * seq_size, total) // tap_rows
    narrow, halves, hubs = width // sources, sources // PAIR, sources + PAIR
    half_width = width // halves
    columns = out_weight.shape[1]
    f32, bf16 = jnp.float32, jnp.bfloat16
    hbm = pl.BlockSpec(memory_space=pl.ANY)
    dma = pltpu.SemaphoreType.DMA
    tables = np.concatenate(block_tables(), axis=0)
    outs = pl.pallas_call(
        block_kernel,
        out_shape=[jax.ShapeDtypeStruct((block_rows // OUTS, columns), f32)] * OUTS,
        in_specs=[hbm] * 6,
        out_specs=[pl.BlockSpec(memory_space=pltpu.VMEM)] * OUTS,
        scratch_shapes=[
            pltpu.VMEM((block_rows, width), f32),
            pltpu.VMEM((block_rows, width), f32),
            pltpu.VMEM((tap_rows, width), f32),
            pltpu.VMEM((1, width), f32),
            pltpu.VMEM((sources, narrow, block_rows), bf16),
            pltpu.VMEM((sources, narrow, tap_rows), bf16),
            pltpu.VMEM((seq_size, narrow, block_rows), bf16),
            pltpu.VMEM((sources, narrow, tap_rows), bf16),
            pltpu.VMEM((seq_size, PAIR, TILE, block_rows), bf16),
            pltpu.VMEM((sources, PAIR, TILE, tap_rows), bf16),
            pltpu.VMEM((total // LANES, narrow, 2 * LANES), f32),
            pltpu.VMEM((total // LANES, narrow, 2 * LANES), f32),
            pltpu.VMEM((total // LANES, narrow, 2 * LANES), f32),
            pltpu.VMEM((seq_size, narrow, block_rows), bf16),
            pltpu.VMEM((seq_size, PAIR, TILE, block_rows), bf16),
            pltpu.VMEM((sources, narrow, block_rows), bf16),
            pltpu.VMEM((ch_size, halves, block_rows, half_width), bf16),
            pltpu.VMEM((ch_size, halves, half_width, columns), bf16),
            pltpu.VMEM(tables.shape, bf16),
            dma((6,)),
            dma((hubs,)),
            dma((seq_size,)),
            dma((hubs,)),
            dma((sources,)),
            dma((seq_size,)),
            dma((hubs,)),
            dma((ch_size, halves)),
            dma((ch_size, halves)),
            pltpu.SemaphoreType.REGULAR((seq_size,)),
            pltpu.SemaphoreType.REGULAR((ch_size,)),
        ],
        compiler_params=pltpu.CompilerParams(
            collective_id=0, has_side_effects=True, vmem_limit_bytes=54500 * 1024
        ),
    )(
        values,
        gates,
        filter_taps,
        skip.reshape(1, width),
        out_weight.reshape(ch_size, halves, half_width, columns),
        jnp.asarray(tables),
    )
    return jnp.concatenate(outs, axis=0)


def local_body(values, gates, filter_taps, skip, out_weight):
    seq_size, ch_size = lax.axis_size("seq"), lax.axis_size("ch")
    block_rows, width = values.shape
    tap_rows = filter_taps.shape[0]
    total = block_rows * seq_size
    sources = min(tap_rows * seq_size, total) // tap_rows
    fits = (
        sources == PAIR * PAIR
        and seq_size % PAIR == 0
        and seq_size >= sources + PAIR
        and width % (sources * TILE) == 0
        and width // sources > TILE
        and width // sources * PAIR % LANES == 0
        and ch_size % 2 == 0
        and block_rows % LANES == 0
        and tap_rows % block_rows == 0
        and sources * block_rows % tap_rows == 0
        and total % tap_rows == 0
        and width // sources * total <= 256 * 1024
    )
    chosen = block_body if fits else body
    return chosen(values, gates, filter_taps, skip, out_weight)


def solution(mesh):
    placed = (P("seq", "ch"), P("seq", "ch"), P("seq", "ch"), P("ch"), P(None, "ch"))
    return jax.shard_map(
        local_body, mesh=mesh, in_specs=placed, out_specs=P("seq", "ch"), check_vma=False
    )
```

```python
import functools
import math

import jax
import jax.numpy as jnp
import numpy as np
from jax import lax
from jax.experimental import pallas as pl
from jax.experimental.pallas import tpu as pltpu
from jax.sharding import PartitionSpec as P

HIGHEST = lax.Precision.HIGHEST
MESH = pl.DeviceIdType.MESH
LANES = 128
TILE = 16
PAIR = 2


def split_length(length):
    leading = 1
    for factor in range(1, math.isqrt(length) + 1):
        if length % factor == 0:
            leading = factor
    return (leading, length // leading)


def phase_table(count_rows, count_cols, modulus):
    row_ids = jnp.arange(count_rows, dtype=jnp.int32)
    col_ids = jnp.arange(count_cols, dtype=jnp.int32)
    wrapped = row_ids[:, None] * col_ids[None, :] % modulus
    phases = 2.0 * math.pi / modulus * wrapped.astype(jnp.float32)
    return (jnp.cos(phases), jnp.sin(phases))


def complex_form(cosine, sine):
    upper = jnp.stack([cosine, -sine], axis=1)
    lower = jnp.stack([sine, cosine], axis=1)
    return jnp.stack([upper, lower], axis=0)


def transform_tables(length):
    rows_lead, rows_tail = split_length(length)
    cos_lead, sin_lead = phase_table(rows_lead, rows_lead, rows_lead)
    cos_tail, sin_tail = phase_table(rows_tail, rows_tail, rows_tail)
    cos_twist, sin_twist = phase_table(rows_lead, rows_tail, length)
    lead_table = jnp.stack([cos_lead, -sin_lead])
    tail_forward = complex_form(cos_tail, -sin_tail)
    tail_inverse = complex_form(cos_tail, sin_tail)
    return (
        lead_table,
        tail_forward,
        tail_inverse,
        cos_twist,
        sin_twist,
        rows_lead,
        rows_tail,
        length,
    )


def twist_rows(section, cosine, sine):
    real_part = section[0] * cosine[None] - section[1] * sine[None]
    imag_part = section[0] * sine[None] + section[1] * cosine[None]
    return jnp.stack([real_part, imag_part])


def forward_rows(rows, tables):
    lead_table, tail_forward, tail_inverse, cos_twist, sin_twist, rows_lead, rows_tail, length = (
        tables
    )
    signal = jnp.concatenate([rows, jnp.zeros_like(rows)], axis=1).reshape(
        rows.shape[0], rows_lead, rows_tail
    )
    section = jnp.einsum("pft,cts->pcfs", lead_table, signal, precision=HIGHEST)
    twisted = twist_rows(section, cos_twist, -sin_twist)
    return jnp.einsum("pgrs,rcfs->pcfg", tail_forward, twisted, precision=HIGHEST)


def inverse_rows(spectrum, tables):
    lead_table, tail_forward, tail_inverse, cos_twist, sin_twist, rows_lead, rows_tail, length = (
        tables
    )
    section = jnp.einsum("pgrs,rcfs->pcfg", tail_inverse, spectrum, precision=HIGHEST)
    twisted = twist_rows(section, cos_twist, sin_twist)
    signal = jnp.einsum("rft,rcfs->cts", lead_table, twisted, precision=HIGHEST) / length
    return signal.reshape(signal.shape[0], length)


def product(left, right):
    real_part = left[0] * right[0] - left[1] * right[1]
    imag_part = left[0] * right[1] + left[1] * right[0]
    return jnp.stack([real_part, imag_part])


def body(values, gates, filter_taps, skip, out_weight):
    block_rows, width = values.shape
    whole_filter = lax.all_gather(filter_taps, "seq", axis=0, tiled=True)
    devices = lax.axis_size("seq")
    narrow = width // devices
    whole_rows = lax.all_to_all(values.T, "seq", split_axis=0, concat_axis=1, tiled=True)
    total_rows = whole_rows.shape[1]
    own_taps = lax.dynamic_slice_in_dim(whole_filter, lax.axis_index("seq") * narrow, narrow, 1).T
    used_taps = min(own_taps.shape[1], total_rows)
    own_taps = own_taps[:, :used_taps]
    taps_rows = jnp.concatenate(
        [own_taps, jnp.zeros((narrow, total_rows - used_taps), jnp.float32)], axis=1
    )
    row_tables = transform_tables(2 * total_rows)
    spectrum = product(forward_rows(whole_rows, row_tables), forward_rows(taps_rows, row_tables))
    convolved_rows = inverse_rows(spectrum, row_tables)[:, :total_rows]
    convolved = lax.all_to_all(convolved_rows, "seq", split_axis=1, concat_axis=0, tiled=True).T
    hidden = (gates * (convolved + skip[None, :] * values)).astype(jnp.bfloat16)
    return jnp.dot(
        lax.all_gather(hidden, "ch", axis=1, tiled=True),
        out_weight,
        preferred_element_type=jnp.float32,
    )


def block_tables():
    size = 2 * LANES
    place = np.arange(size)[:, None]
    odd = 2 * np.arange(LANES)[None, :] + 1
    angle = np.pi / size * (place * odd % (2 * size))
    forward = np.concatenate([np.cos(angle), -np.sin(angle)], axis=1)
    inverse = forward[LANES:].T / LANES

    def two_parts(table, axis):
        high = table.astype(jnp.bfloat16)
        low = (table - high.astype(np.float64)).astype(jnp.bfloat16)
        return np.concatenate([high, low], axis=axis)

    return two_parts(forward, 0), two_parts(inverse, 1)


OUTS = 4


def block_kernel(
    values_hbm,
    gates_hbm,
    taps_hbm,
    skip_hbm,
    weight_hbm,
    tables_hbm,
    out_a,
    out_b,
    out_c,
    out_d,
    values_ref,
    gates_ref,
    taps_ref,
    skip_ref,
    x_out,
    h_out,
    x_in,
    h_in,
    x_tail,
    h_tail,
    x_waves,
    h_waves,
    y_waves,
    y_out,
    y_tail,
    y_in,
    hidden,
    weight,
    tables,
    load_sem,
    x_send,
    x_recv,
    h_send,
    h_recv,
    y_send,
    y_recv,
    g_send,
    g_recv,
    seq_ready,
    ch_ready,
):
    sources, narrow, block_rows = x_out.shape
    seq_size = x_in.shape[0]
    tap_rows = h_out.shape[2]
    ch_size, halves, _, half_width = hidden.shape
    per, pieces = block_rows // LANES, tap_rows // LANES
    hubs, keep = sources + PAIR, narrow - TILE
    early_taps = sources * block_rows // tap_rows
    me, lane_group = lax.axis_index("seq"), lax.axis_index("ch")
    f32, bf16 = jnp.float32, jnp.bfloat16

    loads = [
        pltpu.make_async_copy(source, target, load_sem.at[place])
        for place, (source, target) in enumerate(
            (
                (values_hbm, values_ref),
                (taps_hbm, taps_ref),
                (tables_hbm, tables),
                (gates_hbm, gates_ref),
                (skip_hbm, skip_ref),
                (weight_hbm, weight),
            )
        )
    ]
    for load in loads:
        load.start()

    barrier = pltpu.get_barrier_semaphore()
    for other in range(1, seq_size):
        @pl.when((me < other) & (me < hubs))
        def _():
            pl.semaphore_signal(barrier, inc=1, device_id={"seq": other}, device_id_type=MESH)
    for other in range(1, ch_size):
        @pl.when(lane_group < other)
        def _():
            pl.semaphore_signal(barrier, inc=1, device_id={"ch": other}, device_id_type=MESH)
    earlier = jnp.minimum(me, hubs) + lane_group

    @pl.when(earlier > 0)
    def _():
        pl.semaphore_wait(barrier, earlier)
    for other in range(hubs):
        @pl.when(me > other)
        def _():
            pl.semaphore_signal(
                seq_ready.at[me], inc=1, device_id={"seq": other}, device_id_type=MESH
            )
    for other in range(ch_size - 1):
        @pl.when(lane_group > other)
        def _():
            pl.semaphore_signal(
                ch_ready.at[lane_group], inc=1, device_id={"ch": other}, device_id_type=MESH
            )

    forward, inverse = tables.at[: 4 * LANES], tables.at[4 * LANES :]
    own, rest = pl.ds(0, keep), pl.ds(keep, TILE)

    def transfer(source, target, sends, recvs, to, place):
        return pltpu.make_async_remote_copy(
            source, target, sends.at[to], recvs.at[place],
            device_id={"seq": to}, device_id_type=MESH,
        )

    def tails_of(helper):
        return pl.ds((helper - sources) * PAIR, PAIR)

    def x_copy(to, place, late):
        if to >= sources:
            source, target = x_out.at[tails_of(to), rest], x_tail.at[place]
        elif late:
            source, target = x_out.at[to, own], x_in.at[place, own]
        else:
            source, target = x_out.at[to], x_in.at[place]
        return transfer(source, target, x_send, x_recv, to, place)

    def h_copy(to, place, late):
        if to >= sources:
            source, target = h_out.at[tails_of(to), rest], h_tail.at[place]
        elif late:
            source, target = h_out.at[to, own], h_in.at[place, own]
        else:
            source, target = h_out.at[to], h_in.at[place]
        return transfer(source, target, h_send, h_recv, to, place)

    def y_copy(to, place):
        if to >= sources:
            source, target = y_out.at[to, own], y_in.at[place, own]
        else:
            source, target = y_out.at[to], y_in.at[place]
        return transfer(source, target, y_send, y_recv, to, place)

    def tail_copy(to, helper, place):
        target = y_in.at[pl.ds((helper - sources) * PAIR, PAIR), rest]
        return transfer(y_tail.at[to], target, y_send, y_recv, to, place)

    def ready(to):
        @pl.when(me < to)
        def _():
            pl.semaphore_wait(seq_ready.at[to], 1)

    def send_tails():
        for to in range(sources, hubs):
            pl.semaphore_wait(seq_ready.at[to], 1)
            x_copy(to, me, False).start()
            h_copy(to, me, False).start()

    loads[0].wait()
    x_out[...] = values_ref[...].T.astype(bf16).reshape(x_out.shape)

    @pl.when(me >= sources)
    def _():
        for to in range(hubs):
            if to >= sources:
                ready(to)

            @pl.when(me != to)
            def _():
                x_copy(to, me, True).start()

    loads[1].wait()

    @pl.when(me < sources)
    def _():
        h_out[...] = taps_ref[...].T.astype(bf16).reshape(h_out.shape)
        for to in range(sources):
            ready(to)

            @pl.when(me != to)
            def _():
                x_copy(to, me, False).start()

            @pl.when((me != to) & (me < early_taps))
            def _():
                h_copy(to, me, False).start()

            @pl.when((me != to) & (me >= early_taps))
            def _():
                h_copy(to, me, True).start()

        @pl.when(me >= early_taps)
        def _():
            send_tails()

        x_in[me] = x_out[me]
        h_in[me] = h_out[me]

    loads[2].wait()

    def wait_taps(source, helper):
        late = source >= early_taps
        if helper:
            h_copy(sources, source, late).wait_recv()
        else:
            @pl.when(me != source)
            def _():
                h_copy(0, source, late).wait_recv()

    def wait_values(first, helper):
        for source in range(first, first + PAIR):
            @pl.when(me != source)
            def _():
                x_copy(sources if helper else 0, source, first >= sources).wait_recv()

    def take_taps(source, helper):
        if helper:
            taps, count = h_tail.at[source], PAIR * TILE
        else:
            taps, count = h_in.at[source], keep if source >= early_taps else narrow
        rows = []
        for piece in range(pieces):
            lanes = slice(piece * LANES, (piece + 1) * LANES)
            block = taps[:, :, lanes].reshape(count, LANES) if helper else taps[:count, lanes]
            rows.append(jnp.concatenate([block, block], axis=1))
        table = jnp.concatenate([forward[:LANES], forward[2 * LANES : 3 * LANES]], axis=0)
        waves = jnp.dot(jnp.concatenate(rows, axis=0), table, preferred_element_type=f32)
        h_waves[source * pieces : (source + 1) * pieces, :count] = waves.reshape(
            pieces, count, 2 * LANES
        )

    def take_values(first, helper):
        late = first >= sources
        count = PAIR * TILE if helper else keep if late else narrow
        def piece_of(source, piece):
            lanes = slice(piece * LANES, (piece + 1) * LANES)
            if helper:
                return x_tail[source, :, :, lanes].reshape(count, LANES)
            return x_in[source, :count, lanes]

        before = piece_of(first - 1, per - 1) if first else jnp.zeros((count, LANES), bf16)
        rows = []
        for source in range(first, first + PAIR):
            for piece in range(per):
                here = piece_of(source, piece)
                rows.append(jnp.concatenate([before, here, before, here], axis=1))
                before = here
        waves = jnp.dot(
            jnp.concatenate(rows, axis=0), forward[...], preferred_element_type=f32
        )
        x_waves[first * per : (first + PAIR) * per, :count] = waves.reshape(
            PAIR * per, count, 2 * LANES
        )

    def multiply(first, low, high, fresh, tiles):
        start, count = first * per, PAIR * per

        def one(part, carry):
            rows = pl.ds(pl.multiple_of(part * TILE, TILE), TILE)
            real_lanes, imag_lanes = slice(0, LANES), slice(LANES, 2 * LANES)
            cache = {}

            def x_part(block):
                if block not in cache:
                    cache[block] = (
                        x_waves[block, rows, real_lanes], x_waves[block, rows, imag_lanes]
                    )
                return cache[block]

            sums = [None] * count
            if not fresh:
                sums = [
                    (y_waves[start + spot, rows, real_lanes], y_waves[start + spot, rows, imag_lanes])
                    for spot in range(count)
                ]
            for lag in range(max(0, start - high + 1), start + count - low):
                h_real, h_imag = h_waves[lag, rows, real_lanes], h_waves[lag, rows, imag_lanes]
                for spot in range(count):
                    block = start + spot - lag
                    if not low <= block < high:
                        continue
                    x_real, x_imag = x_part(block)
                    real = x_real * h_real - x_imag * h_imag
                    imag = x_real * h_imag + x_imag * h_real
                    if sums[spot] is not None:
                        real, imag = sums[spot][0] + real, sums[spot][1] + imag
                    sums[spot] = (real, imag)
            for spot in range(count):
                y_waves[start + spot, rows, real_lanes] = sums[spot][0]
                y_waves[start + spot, rows, imag_lanes] = sums[spot][1]
            return carry

        lax.fori_loop(0, tiles, one, 0)

    def give_back(first, helper):
        count = PAIR * TILE if helper else keep if first >= sources else narrow
        waves = y_waves[first * per : (first + PAIR) * per, :count].reshape(
            PAIR * per * count, 2 * LANES
        )
        high = waves.astype(bf16)
        low = (waves - high.astype(f32)).astype(bf16)
        both = jnp.dot(high, inverse[...], preferred_element_type=f32)
        more = jnp.dot(low, inverse[:, :LANES], preferred_element_type=f32)
        convolved = (both[:, :LANES] + both[:, LANES:] + more).astype(bf16)
        for spot in range(PAIR * per):
            to, piece = first + spot // per, spot % per
            lanes = slice(piece * LANES, (piece + 1) * LANES)
            part = convolved[spot * count : (spot + 1) * count]
            if helper:
                y_tail[to, :, :, lanes] = part.reshape(PAIR, TILE, LANES)
            else:
                y_out[to, :count, lanes] = part
        for to in range(first, first + PAIR):
            if to >= hubs:
                pl.semaphore_wait(seq_ready.at[to], 1)
            if not helper:
                @pl.when(me != to)
                def _():
                    y_copy(to, me).start()
            else:
                for which in range(sources, hubs):
                    @pl.when((me == which) & (me != to))
                    def _():
                        tail_copy(to, which, me).start()

    def convolve_own():
        taken = 0
        for first in range(0, sources, PAIR):
            fresh = taken
            while taken < early_taps and taken * tap_rows < (first + PAIR) * block_rows:
                wait_taps(taken, False)
                taken += 1
            wait_values(first, False)
            if not first:
                @pl.when(me < early_taps)
                def _():
                    send_tails()

            for source in range(fresh, taken):
                take_taps(source, False)
            take_values(first, False)
            multiply(first, 0, (first + PAIR) * per, True, narrow // TILE)
            give_back(first, False)
        tiles = keep // TILE
        for source in range(early_taps, sources):
            wait_taps(source, False)
        for source in range(early_taps, sources):
            take_taps(source, False)
        for first in range(sources, seq_size, PAIR):
            multiply(first, 0, sources * per, True, tiles)
        for first in range(sources, seq_size, PAIR):
            wait_values(first, False)
        for first in range(sources, seq_size, PAIR):
            take_values(first, False)
        for first in range(sources, seq_size, PAIR):
            multiply(first, sources * per, (first + PAIR) * per, False, tiles)
            give_back(first, False)

    def convolve_tails():
        for first in range(PAIR, seq_size, PAIR):
            wait_values(first, True)
            if first >= sources:
                take_values(first, True)
        for source in range(early_taps, sources):
            wait_taps(source, True)
            take_taps(source, True)
        wait_values(0, True)
        for source in range(early_taps):
            wait_taps(source, True)
        for first in range(0, sources, PAIR):
            take_values(first, True)
        for source in range(early_taps):
            take_taps(source, True)
        for first in range(sources, seq_size, PAIR):
            multiply(first, 0, (first + PAIR) * per, True, PAIR)
            give_back(first, True)

    @pl.when(me < sources)
    def _():
        convolve_own()
        y_in[me] = y_out[me]

    for which in range(sources, hubs):
        @pl.when(me == which)
        def _():
            tails = slice((which - sources) * PAIR, (which - sources + 1) * PAIR)
            x_tail[which] = x_out[tails, keep:]

    @pl.when((me >= sources) & (me < hubs))
    def _():
        convolve_tails()

    for which in range(sources, hubs):
        @pl.when(me == which)
        def _():
            tails = slice((which - sources) * PAIR, (which - sources + 1) * PAIR)
            y_in[tails, keep:] = y_tail[which]

    partner = lane_group + 1 - 2 * lax.rem(lane_group, 2)
    pairs = ch_size // 2

    def spread(kind, half, slot, to):
        block = hidden.at[slot, half]
        copy = pltpu.make_async_remote_copy(
            block, block, g_send.at[kind, half], g_recv.at[kind, half],
            device_id={"ch": to}, device_id_type=MESH,
        )
        copy.start()
        g_copies.append(copy)
        return copy

    def add_product(half, slot, first=False):
        term = jnp.dot(hidden[slot, half], weight[slot, half], preferred_element_type=f32)
        for place, out in enumerate(outs):
            part = term[place * out_rows : (place + 1) * out_rows]
            out[...] = part if first else out[...] + part

    for other in range(1, ch_size):
        @pl.when(lane_group < other)
        def _():
            pl.semaphore_wait(ch_ready.at[other], 1)

    outs = (out_a, out_b, out_c, out_d)
    out_rows = out_a.shape[0]
    g_copies, direct, relayed = [], {}, {}
    for load in loads[3:5]:
        load.wait()
    for half in range(halves):
        for part in range(PAIR):
            source = half * PAIR + part

            @pl.when((me != source) & (me < sources))
            def _():
                y_copy(0, source).wait_recv()

            @pl.when(me >= sources)
            def _():
                y_copy(sources, source).wait_recv()

        @pl.when((me >= sources) & (me != sources + half))
        def _():
            tail_copy(sources, sources, sources + half).wait_recv()
        convolved = y_in[half * PAIR : (half + 1) * PAIR].astype(f32).reshape(half_width, block_rows).T
        span = slice(half * half_width, (half + 1) * half_width)
        hidden[lane_group, half] = (
            gates_ref[:, span] * (convolved + skip_ref[:, span] * values_ref[:, span])
        ).astype(bf16)
        for pair in range(1, pairs):
            direct[pair, half] = spread(
                2 * pair - 1, half, lane_group, lax.rem(lane_group + 2 * pair, ch_size)
            )
            if half == halves - 1:
                relayed[pair, half] = spread(
                    2 * pair, half, lane_group, lax.rem(partner + 2 * pair, ch_size)
                )
        direct[0, half] = spread(0, half, lane_group, partner)
    loads[5].wait()
    for half in range(halves):
        add_product(half, lane_group, not half)
    for half in range(halves):
        direct[0, half].wait_recv()
        add_product(half, partner)
        for pair in range(1, pairs):
            slot = lax.rem(lane_group + ch_size - 2 * pair, ch_size)
            direct[pair, half].wait_recv()
            if half < halves - 1:
                relayed[pair, half] = spread(2 * pair, half, slot, partner)
            add_product(half, slot)
    for half in range(halves):
        for pair in range(1, pairs):
            slot = lax.rem(partner + ch_size - 2 * pair, ch_size)
            relayed[pair, half].wait_recv()
            add_product(half, slot)

    for copy in g_copies:
        copy.wait_send()
    for to in range(hubs):
        for late in (False, True):
            @pl.when((me != to) & ((me >= sources) == late))
            def _():
                x_copy(to, me, late).wait_send()

            @pl.when((me != to) & (me < sources) & ((me >= early_taps) == late))
            def _():
                h_copy(to, me, late).wait_send()
    for to in range(seq_size):
        @pl.when((me != to) & (me < sources))
        def _():
            y_copy(to, me).wait_send()

        if to >= sources:
            @pl.when((me != to) & (me >= sources) & (me < hubs))
            def _():
                tail_copy(to, sources, me).wait_send()


def block_body(values, gates, filter_taps, skip, out_weight):
    seq_size, ch_size = lax.axis_size("seq"), lax.axis_size("ch")
    block_rows, width = values.shape
    tap_rows = filter_taps.shape[0]
    total = block_rows * seq_size
    sources = min(tap_rows * seq_size, total) // tap_rows
    narrow, halves, hubs = width // sources, sources // PAIR, sources + PAIR
    half_width = width // halves
    columns = out_weight.shape[1]
    f32, bf16 = jnp.float32, jnp.bfloat16
    hbm = pl.BlockSpec(memory_space=pl.ANY)
    dma = pltpu.SemaphoreType.DMA
    tables = np.concatenate(block_tables(), axis=0)
    outs = pl.pallas_call(
        block_kernel,
        out_shape=[jax.ShapeDtypeStruct((block_rows // OUTS, columns), f32)] * OUTS,
        in_specs=[hbm] * 6,
        out_specs=[pl.BlockSpec(memory_space=pltpu.VMEM)] * OUTS,
        scratch_shapes=[
            pltpu.VMEM((block_rows, width), f32),
            pltpu.VMEM((block_rows, width), f32),
            pltpu.VMEM((tap_rows, width), f32),
            pltpu.VMEM((1, width), f32),
            pltpu.VMEM((sources, narrow, block_rows), bf16),
            pltpu.VMEM((sources, narrow, tap_rows), bf16),
            pltpu.VMEM((seq_size, narrow, block_rows), bf16),
            pltpu.VMEM((sources, narrow, tap_rows), bf16),
            pltpu.VMEM((seq_size, PAIR, TILE, block_rows), bf16),
            pltpu.VMEM((sources, PAIR, TILE, tap_rows), bf16),
            pltpu.VMEM((total // LANES, narrow, 2 * LANES), f32),
            pltpu.VMEM((total // LANES, narrow, 2 * LANES), f32),
            pltpu.VMEM((total // LANES, narrow, 2 * LANES), f32),
            pltpu.VMEM((seq_size, narrow, block_rows), bf16),
            pltpu.VMEM((seq_size, PAIR, TILE, block_rows), bf16),
            pltpu.VMEM((sources, narrow, block_rows), bf16),
            pltpu.VMEM((ch_size, halves, block_rows, half_width), bf16),
            pltpu.VMEM((ch_size, halves, half_width, columns), bf16),
            pltpu.VMEM(tables.shape, bf16),
            dma((6,)),
            dma((hubs,)),
            dma((seq_size,)),
            dma((hubs,)),
            dma((sources,)),
            dma((seq_size,)),
            dma((hubs,)),
            dma((ch_size, halves)),
            dma((ch_size, halves)),
            pltpu.SemaphoreType.REGULAR((seq_size,)),
            pltpu.SemaphoreType.REGULAR((ch_size,)),
        ],
        compiler_params=pltpu.CompilerParams(
            collective_id=0, has_side_effects=True, vmem_limit_bytes=54500 * 1024
        ),
    )(
        values,
        gates,
        filter_taps,
        skip.reshape(1, width),
        out_weight.reshape(ch_size, halves, half_width, columns),
        jnp.asarray(tables),
    )
    return jnp.concatenate(outs, axis=0)


def local_body(values, gates, filter_taps, skip, out_weight):
    seq_size, ch_size = lax.axis_size("seq"), lax.axis_size("ch")
    block_rows, width = values.shape
    tap_rows = filter_taps.shape[0]
    total = block_rows * seq_size
    sources = min(tap_rows * seq_size, total) // tap_rows
    fits = (
        sources == PAIR * PAIR
        and seq_size % PAIR == 0
        and seq_size >= sources + PAIR
        and width % (sources * TILE) == 0
        and width // sources > TILE
        and width // sources * PAIR % LANES == 0
        and ch_size % 2 == 0
        and block_rows % LANES == 0
        and tap_rows % block_rows == 0
        and sources * block_rows % tap_rows == 0
        and total % tap_rows == 0
        and width // sources * total <= 256 * 1024
    )
    chosen = block_body if fits else body
    return chosen(values, gates, filter_taps, skip, out_weight)


def solution(mesh):
    placed = (P("seq", "ch"), P("seq", "ch"), P("seq", "ch"), P("ch"), P(None, "ch"))
    return jax.shard_map(
        local_body, mesh=mesh, in_specs=placed, out_specs=P("seq", "ch"), check_vma=False
    )
```

```python
import functools
import math

import jax
import jax.numpy as jnp
import numpy as np
from jax import lax
from jax.experimental import pallas as pl
from jax.experimental.pallas import tpu as pltpu
from jax.sharding import PartitionSpec as P

HIGHEST = lax.Precision.HIGHEST
MESH = pl.DeviceIdType.MESH
LANES = 128
TILE = 16
PAIR = 2


def split_length(length):
    leading = 1
    for factor in range(1, math.isqrt(length) + 1):
        if length % factor == 0:
            leading = factor
    return (leading, length // leading)


def phase_table(count_rows, count_cols, modulus):
    row_ids = jnp.arange(count_rows, dtype=jnp.int32)
    col_ids = jnp.arange(count_cols, dtype=jnp.int32)
    wrapped = row_ids[:, None] * col_ids[None, :] % modulus
    phases = 2.0 * math.pi / modulus * wrapped.astype(jnp.float32)
    return (jnp.cos(phases), jnp.sin(phases))


def complex_form(cosine, sine):
    upper = jnp.stack([cosine, -sine], axis=1)
    lower = jnp.stack([sine, cosine], axis=1)
    return jnp.stack([upper, lower], axis=0)


def transform_tables(length):
    rows_lead, rows_tail = split_length(length)
    cos_lead, sin_lead = phase_table(rows_lead, rows_lead, rows_lead)
    cos_tail, sin_tail = phase_table(rows_tail, rows_tail, rows_tail)
    cos_twist, sin_twist = phase_table(rows_lead, rows_tail, length)
    lead_table = jnp.stack([cos_lead, -sin_lead])
    tail_forward = complex_form(cos_tail, -sin_tail)
    tail_inverse = complex_form(cos_tail, sin_tail)
    return (
        lead_table,
        tail_forward,
        tail_inverse,
        cos_twist,
        sin_twist,
        rows_lead,
        rows_tail,
        length,
    )


def twist_rows(section, cosine, sine):
    real_part = section[0] * cosine[None] - section[1] * sine[None]
    imag_part = section[0] * sine[None] + section[1] * cosine[None]
    return jnp.stack([real_part, imag_part])


def forward_rows(rows, tables):
    lead_table, tail_forward, tail_inverse, cos_twist, sin_twist, rows_lead, rows_tail, length = (
        tables
    )
    signal = jnp.concatenate([rows, jnp.zeros_like(rows)], axis=1).reshape(
        rows.shape[0], rows_lead, rows_tail
    )
    section = jnp.einsum("pft,cts->pcfs", lead_table, signal, precision=HIGHEST)
    twisted = twist_rows(section, cos_twist, -sin_twist)
    return jnp.einsum("pgrs,rcfs->pcfg", tail_forward, twisted, precision=HIGHEST)


def inverse_rows(spectrum, tables):
    lead_table, tail_forward, tail_inverse, cos_twist, sin_twist, rows_lead, rows_tail, length = (
        tables
    )
    section = jnp.einsum("pgrs,rcfs->pcfg", tail_inverse, spectrum, precision=HIGHEST)
    twisted = twist_rows(section, cos_twist, sin_twist)
    signal = jnp.einsum("rft,rcfs->cts", lead_table, twisted, precision=HIGHEST) / length
    return signal.reshape(signal.shape[0], length)


def product(left, right):
    real_part = left[0] * right[0] - left[1] * right[1]
    imag_part = left[0] * right[1] + left[1] * right[0]
    return jnp.stack([real_part, imag_part])


def body(values, gates, filter_taps, skip, out_weight):
    block_rows, width = values.shape
    whole_filter = lax.all_gather(filter_taps, "seq", axis=0, tiled=True)
    devices = lax.axis_size("seq")
    narrow = width // devices
    whole_rows = lax.all_to_all(values.T, "seq", split_axis=0, concat_axis=1, tiled=True)
    total_rows = whole_rows.shape[1]
    own_taps = lax.dynamic_slice_in_dim(whole_filter, lax.axis_index("seq") * narrow, narrow, 1).T
    used_taps = min(own_taps.shape[1], total_rows)
    own_taps = own_taps[:, :used_taps]
    taps_rows = jnp.concatenate(
        [own_taps, jnp.zeros((narrow, total_rows - used_taps), jnp.float32)], axis=1
    )
    row_tables = transform_tables(2 * total_rows)
    spectrum = product(forward_rows(whole_rows, row_tables), forward_rows(taps_rows, row_tables))
    convolved_rows = inverse_rows(spectrum, row_tables)[:, :total_rows]
    convolved = lax.all_to_all(convolved_rows, "seq", split_axis=1, concat_axis=0, tiled=True).T
    hidden = (gates * (convolved + skip[None, :] * values)).astype(jnp.bfloat16)
    return jnp.dot(
        lax.all_gather(hidden, "ch", axis=1, tiled=True),
        out_weight,
        preferred_element_type=jnp.float32,
    )


def block_tables():
    size = 2 * LANES
    place = np.arange(size)[:, None]
    odd = 2 * np.arange(LANES)[None, :] + 1
    angle = np.pi / size * (place * odd % (2 * size))
    forward = np.concatenate([np.cos(angle), -np.sin(angle)], axis=1)
    inverse = forward[LANES:].T / LANES

    def two_parts(table, axis):
        high = table.astype(jnp.bfloat16)
        low = (table - high.astype(np.float64)).astype(jnp.bfloat16)
        return np.concatenate([high, low], axis=axis)

    return two_parts(forward, 0), two_parts(inverse, 1)


OUTS = 4


def block_kernel(
    values_hbm,
    gates_hbm,
    taps_hbm,
    skip_hbm,
    weight_hbm,
    tables_hbm,
    out_a,
    out_b,
    out_c,
    out_d,
    values_ref,
    gates_ref,
    taps_ref,
    skip_ref,
    x_out,
    h_out,
    x_in,
    h_in,
    x_tail,
    h_tail,
    x_waves,
    h_waves,
    y_waves,
    y_out,
    y_tail,
    y_in,
    hidden,
    weight,
    tables,
    load_sem,
    x_send,
    x_recv,
    h_send,
    h_recv,
    y_send,
    y_recv,
    g_send,
    g_recv,
    seq_ready,
    ch_ready,
):
    sources, narrow, block_rows = x_out.shape
    seq_size = x_in.shape[0]
    tap_rows = h_out.shape[2]
    ch_size, halves, _, half_width = hidden.shape
    per, pieces = block_rows // LANES, tap_rows // LANES
    hubs, keep = sources + PAIR, narrow - TILE
    early_taps = sources * block_rows // tap_rows
    me, lane_group = lax.axis_index("seq"), lax.axis_index("ch")
    f32, bf16 = jnp.float32, jnp.bfloat16

    loads = [
        pltpu.make_async_copy(source, target, load_sem.at[place])
        for place, (source, target) in enumerate(
            (
                (values_hbm, values_ref),
                (taps_hbm, taps_ref),
                (tables_hbm, tables),
                (gates_hbm, gates_ref),
                (skip_hbm, skip_ref),
                (weight_hbm, weight),
            )
        )
    ]
    for load in loads:
        load.start()

    barrier = pltpu.get_barrier_semaphore()
    for other in range(1, seq_size):
        @pl.when((me < other) & (me < hubs))
        def _():
            pl.semaphore_signal(barrier, inc=1, device_id={"seq": other}, device_id_type=MESH)
    for other in range(1, ch_size):
        @pl.when(lane_group < other)
        def _():
            pl.semaphore_signal(barrier, inc=1, device_id={"ch": other}, device_id_type=MESH)
    earlier = jnp.minimum(me, hubs) + lane_group

    @pl.when(earlier > 0)
    def _():
        pl.semaphore_wait(barrier, earlier)
    for other in range(hubs):
        @pl.when(me > other)
        def _():
            pl.semaphore_signal(
                seq_ready.at[me], inc=1, device_id={"seq": other}, device_id_type=MESH
            )
    for other in range(ch_size - 1):
        @pl.when(lane_group > other)
        def _():
            pl.semaphore_signal(
                ch_ready.at[lane_group], inc=1, device_id={"ch": other}, device_id_type=MESH
            )

    forward, inverse = tables.at[: 4 * LANES], tables.at[4 * LANES :]
    own, rest = pl.ds(0, keep), pl.ds(keep, TILE)

    def transfer(source, target, sends, recvs, to, place):
        return pltpu.make_async_remote_copy(
            source, target, sends.at[to], recvs.at[place],
            device_id={"seq": to}, device_id_type=MESH,
        )

    def tails_of(helper):
        return pl.ds((helper - sources) * PAIR, PAIR)

    def x_copy(to, place, late):
        if to >= sources:
            source, target = x_out.at[tails_of(to), rest], x_tail.at[place]
        elif late:
            source, target = x_out.at[to, own], x_in.at[place, own]
        else:
            source, target = x_out.at[to], x_in.at[place]
        return transfer(source, target, x_send, x_recv, to, place)

    def h_copy(to, place, late):
        if to >= sources:
            source, target = h_out.at[tails_of(to), rest], h_tail.at[place]
        elif late:
            source, target = h_out.at[to, own], h_in.at[place, own]
        else:
            source, target = h_out.at[to], h_in.at[place]
        return transfer(source, target, h_send, h_recv, to, place)

    def y_copy(to, place):
        if to >= sources:
            source, target = y_out.at[to, own], y_in.at[place, own]
        else:
            source, target = y_out.at[to], y_in.at[place]
        return transfer(source, target, y_send, y_recv, to, place)

    def tail_copy(to, helper, place):
        target = y_in.at[pl.ds((helper - sources) * PAIR, PAIR), rest]
        return transfer(y_tail.at[to], target, y_send, y_recv, to, place)

    def ready(to):
        @pl.when(me < to)
        def _():
            pl.semaphore_wait(seq_ready.at[to], 1)

    def send_tails():
        for to in range(sources, hubs):
            pl.semaphore_wait(seq_ready.at[to], 1)
            x_copy(to, me, False).start()
            h_copy(to, me, False).start()

    loads[0].wait()
    x_out[...] = values_ref[...].T.astype(bf16).reshape(x_out.shape)

    @pl.when(me >= sources)
    def _():
        for to in range(hubs):
            if to >= sources:
                ready(to)

            @pl.when(me != to)
            def _():
                x_copy(to, me, True).start()

    loads[1].wait()

    @pl.when(me < sources)
    def _():
        h_out[...] = taps_ref[...].T.astype(bf16).reshape(h_out.shape)
        for to in range(sources):
            ready(to)

            @pl.when(me != to)
            def _():
                x_copy(to, me, False).start()

            @pl.when((me != to) & (me < early_taps))
            def _():
                h_copy(to, me, False).start()

            @pl.when((me != to) & (me >= early_taps))
            def _():
                h_copy(to, me, True).start()

        @pl.when(me >= early_taps)
        def _():
            send_tails()

        x_in[me] = x_out[me]
        h_in[me] = h_out[me]

    loads[2].wait()

    def wait_taps(source, helper):
        late = source >= early_taps
        if helper:
            h_copy(sources, source, late).wait_recv()
        else:
            @pl.when(me != source)
            def _():
                h_copy(0, source, late).wait_recv()

    def wait_values(first, helper):
        for source in range(first, first + PAIR):
            @pl.when(me != source)
            def _():
                x_copy(sources if helper else 0, source, first >= sources).wait_recv()

    def take_taps(source, helper):
        if helper:
            taps, count = h_tail.at[source], PAIR * TILE
        else:
            taps, count = h_in.at[source], keep if source >= early_taps else narrow
        rows = []
        for piece in range(pieces):
            lanes = slice(piece * LANES, (piece + 1) * LANES)
            block = taps[:, :, lanes].reshape(count, LANES) if helper else taps[:count, lanes]
            rows.append(jnp.concatenate([block, block], axis=1))
        table = jnp.concatenate([forward[:LANES], forward[2 * LANES : 3 * LANES]], axis=0)
        waves = jnp.dot(jnp.concatenate(rows, axis=0), table, preferred_element_type=f32)
        h_waves[source * pieces : (source + 1) * pieces, :count] = waves.reshape(
            pieces, count, 2 * LANES
        )

    def take_values(first, helper):
        late = first >= sources
        count = PAIR * TILE if helper else keep if late else narrow
        def piece_of(source, piece):
            lanes = slice(piece * LANES, (piece + 1) * LANES)
            if helper:
                return x_tail[source, :, :, lanes].reshape(count, LANES)
            return x_in[source, :count, lanes]

        before = piece_of(first - 1, per - 1) if first else jnp.zeros((count, LANES), bf16)
        rows = []
        for source in range(first, first + PAIR):
            for piece in range(per):
                here = piece_of(source, piece)
                rows.append(jnp.concatenate([before, here, before, here], axis=1))
                before = here
        waves = jnp.dot(
            jnp.concatenate(rows, axis=0), forward[...], preferred_element_type=f32
        )
        x_waves[first * per : (first + PAIR) * per, :count] = waves.reshape(
            PAIR * per, count, 2 * LANES
        )

    def multiply(first, low, high, fresh, tiles):
        start, count = first * per, PAIR * per

        def one(part, carry):
            rows = pl.ds(pl.multiple_of(part * TILE, TILE), TILE)
            real_lanes, imag_lanes = slice(0, LANES), slice(LANES, 2 * LANES)
            cache = {}

            def x_part(block):
                if block not in cache:
                    cache[block] = (
                        x_waves[block, rows, real_lanes], x_waves[block, rows, imag_lanes]
                    )
                return cache[block]

            sums = [None] * count
            if not fresh:
                sums = [
                    (y_waves[start + spot, rows, real_lanes], y_waves[start + spot, rows, imag_lanes])
                    for spot in range(count)
                ]
            for lag in range(max(0, start - high + 1), start + count - low):
                h_real, h_imag = h_waves[lag, rows, real_lanes], h_waves[lag, rows, imag_lanes]
                for spot in range(count):
                    block = start + spot - lag
                    if not low <= block < high:
                        continue
                    x_real, x_imag = x_part(block)
                    real = x_real * h_real - x_imag * h_imag
                    imag = x_real * h_imag + x_imag * h_real
                    if sums[spot] is not None:
                        real, imag = sums[spot][0] + real, sums[spot][1] + imag
                    sums[spot] = (real, imag)
            for spot in range(count):
                y_waves[start + spot, rows, real_lanes] = sums[spot][0]
                y_waves[start + spot, rows, imag_lanes] = sums[spot][1]
            return carry

        lax.fori_loop(0, tiles, one, 0)

    def give_back(first, helper):
        count = PAIR * TILE if helper else keep if first >= sources else narrow
        waves = y_waves[first * per : (first + PAIR) * per, :count].reshape(
            PAIR * per * count, 2 * LANES
        )
        high = waves.astype(bf16)
        low = (waves - high.astype(f32)).astype(bf16)
        both = jnp.dot(high, inverse[...], preferred_element_type=f32)
        more = jnp.dot(low, inverse[:, :LANES], preferred_element_type=f32)
        convolved = (both[:, :LANES] + both[:, LANES:] + more).astype(bf16)
        for spot in range(PAIR * per):
            to, piece = first + spot // per, spot % per
            lanes = slice(piece * LANES, (piece + 1) * LANES)
            part = convolved[spot * count : (spot + 1) * count]
            if helper:
                y_tail[to, :, :, lanes] = part.reshape(PAIR, TILE, LANES)
            else:
                y_out[to, :count, lanes] = part
        for to in range(first, first + PAIR):
            if to >= hubs:
                pl.semaphore_wait(seq_ready.at[to], 1)
            if not helper:
                @pl.when(me != to)
                def _():
                    y_copy(to, me).start()
            else:
                for which in range(sources, hubs):
                    @pl.when((me == which) & (me != to))
                    def _():
                        tail_copy(to, which, me).start()

    def convolve_own():
        taken = 0
        for first in range(0, sources, PAIR):
            fresh = taken
            while taken < early_taps and taken * tap_rows < (first + PAIR) * block_rows:
                wait_taps(taken, False)
                taken += 1
            wait_values(first, False)
            if not first:
                @pl.when(me < early_taps)
                def _():
                    send_tails()

            for source in range(fresh, taken):
                take_taps(source, False)
            take_values(first, False)
            multiply(first, 0, (first + PAIR) * per, True, narrow // TILE)
            give_back(first, False)
        tiles = keep // TILE
        for source in range(early_taps, sources):
            wait_taps(source, False)
        for source in range(early_taps, sources):
            take_taps(source, False)
        for first in range(sources, seq_size, PAIR):
            multiply(first, 0, sources * per, True, tiles)
        for first in range(sources, seq_size, PAIR):
            wait_values(first, False)
        for first in range(sources, seq_size, PAIR):
            take_values(first, False)
        for first in range(sources, seq_size, PAIR):
            multiply(first, sources * per, (first + PAIR) * per, False, tiles)
            give_back(first, False)

    def convolve_tails():
        for first in range(PAIR, seq_size, PAIR):
            wait_values(first, True)
            if first >= sources:
                take_values(first, True)
        for source in range(early_taps, sources):
            wait_taps(source, True)
            take_taps(source, True)
        wait_values(0, True)
        for source in range(early_taps):
            wait_taps(source, True)
        for first in range(0, sources, PAIR):
            take_values(first, True)
        for source in range(early_taps):
            take_taps(source, True)
        for first in range(seq_size - PAIR, sources - 1, -PAIR):
            multiply(first, 0, (first + PAIR) * per, True, PAIR)
            give_back(first, True)

    @pl.when(me < sources)
    def _():
        convolve_own()
        y_in[me] = y_out[me]

    for which in range(sources, hubs):
        @pl.when(me == which)
        def _():
            tails = slice((which - sources) * PAIR, (which - sources + 1) * PAIR)
            x_tail[which] = x_out[tails, keep:]

    @pl.when((me >= sources) & (me < hubs))
    def _():
        convolve_tails()

    for which in range(sources, hubs):
        @pl.when(me == which)
        def _():
            tails = slice((which - sources) * PAIR, (which - sources + 1) * PAIR)
            y_in[tails, keep:] = y_tail[which]

    partner = lane_group + 1 - 2 * lax.rem(lane_group, 2)
    pairs = ch_size // 2

    def spread(kind, half, slot, to):
        block = hidden.at[slot, half]
        copy = pltpu.make_async_remote_copy(
            block, block, g_send.at[kind, half], g_recv.at[kind, half],
            device_id={"ch": to}, device_id_type=MESH,
        )
        copy.start()
        g_copies.append(copy)
        return copy

    def add_product(half, slot, first=False):
        term = jnp.dot(hidden[slot, half], weight[slot, half], preferred_element_type=f32)
        for place, out in enumerate(outs):
            part = term[place * out_rows : (place + 1) * out_rows]
            out[...] = part if first else out[...] + part

    for other in range(1, ch_size):
        @pl.when(lane_group < other)
        def _():
            pl.semaphore_wait(ch_ready.at[other], 1)

    outs = (out_a, out_b, out_c, out_d)
    out_rows = out_a.shape[0]
    g_copies, direct, relayed = [], {}, {}
    for load in loads[3:5]:
        load.wait()
    for half in range(halves):
        for part in range(PAIR):
            source = half * PAIR + part

            @pl.when((me != source) & (me < sources))
            def _():
                y_copy(0, source).wait_recv()

            @pl.when(me >= sources)
            def _():
                y_copy(sources, source).wait_recv()

        @pl.when((me >= sources) & (me != sources + half))
        def _():
            tail_copy(sources, sources, sources + half).wait_recv()
        convolved = y_in[half * PAIR : (half + 1) * PAIR].astype(f32).reshape(half_width, block_rows).T
        span = slice(half * half_width, (half + 1) * half_width)
        hidden[lane_group, half] = (
            gates_ref[:, span] * (convolved + skip_ref[:, span] * values_ref[:, span])
        ).astype(bf16)
        for pair in range(1, pairs):
            direct[pair, half] = spread(
                2 * pair - 1, half, lane_group, lax.rem(lane_group + 2 * pair, ch_size)
            )
            if half == halves - 1:
                relayed[pair, half] = spread(
                    2 * pair, half, lane_group, lax.rem(partner + 2 * pair, ch_size)
                )
        direct[0, half] = spread(0, half, lane_group, partner)
    loads[5].wait()
    for half in range(halves):
        add_product(half, lane_group, not half)
    for half in range(halves):
        direct[0, half].wait_recv()
        add_product(half, partner)
        for pair in range(1, pairs):
            slot = lax.rem(lane_group + ch_size - 2 * pair, ch_size)
            direct[pair, half].wait_recv()
            if half < halves - 1:
                relayed[pair, half] = spread(2 * pair, half, slot, partner)
            add_product(half, slot)
    for half in range(halves):
        for pair in range(1, pairs):
            slot = lax.rem(partner + ch_size - 2 * pair, ch_size)
            relayed[pair, half].wait_recv()
            add_product(half, slot)

    for copy in g_copies:
        copy.wait_send()
    for to in range(hubs):
        for late in (False, True):
            @pl.when((me != to) & ((me >= sources) == late))
            def _():
                x_copy(to, me, late).wait_send()

            @pl.when((me != to) & (me < sources) & ((me >= early_taps) == late))
            def _():
                h_copy(to, me, late).wait_send()
    for to in range(seq_size):
        @pl.when((me != to) & (me < sources))
        def _():
            y_copy(to, me).wait_send()

        if to >= sources:
            @pl.when((me != to) & (me >= sources) & (me < hubs))
            def _():
                tail_copy(to, sources, me).wait_send()


def block_body(values, gates, filter_taps, skip, out_weight):
    seq_size, ch_size = lax.axis_size("seq"), lax.axis_size("ch")
    block_rows, width = values.shape
    tap_rows = filter_taps.shape[0]
    total = block_rows * seq_size
    sources = min(tap_rows * seq_size, total) // tap_rows
    narrow, halves, hubs = width // sources, sources // PAIR, sources + PAIR
    half_width = width // halves
    columns = out_weight.shape[1]
    f32, bf16 = jnp.float32, jnp.bfloat16
    hbm = pl.BlockSpec(memory_space=pl.ANY)
    dma = pltpu.SemaphoreType.DMA
    tables = np.concatenate(block_tables(), axis=0)
    outs = pl.pallas_call(
        block_kernel,
        out_shape=[jax.ShapeDtypeStruct((block_rows // OUTS, columns), f32)] * OUTS,
        in_specs=[hbm] * 6,
        out_specs=[pl.BlockSpec(memory_space=pltpu.VMEM)] * OUTS,
        scratch_shapes=[
            pltpu.VMEM((block_rows, width), f32),
            pltpu.VMEM((block_rows, width), f32),
            pltpu.VMEM((tap_rows, width), f32),
            pltpu.VMEM((1, width), f32),
            pltpu.VMEM((sources, narrow, block_rows), bf16),
            pltpu.VMEM((sources, narrow, tap_rows), bf16),
            pltpu.VMEM((seq_size, narrow, block_rows), bf16),
            pltpu.VMEM((sources, narrow, tap_rows), bf16),
            pltpu.VMEM((seq_size, PAIR, TILE, block_rows), bf16),
            pltpu.VMEM((sources, PAIR, TILE, tap_rows), bf16),
            pltpu.VMEM((total // LANES, narrow, 2 * LANES), f32),
            pltpu.VMEM((total // LANES, narrow, 2 * LANES), f32),
            pltpu.VMEM((total // LANES, narrow, 2 * LANES), f32),
            pltpu.VMEM((seq_size, narrow, block_rows), bf16),
            pltpu.VMEM((seq_size, PAIR, TILE, block_rows), bf16),
            pltpu.VMEM((sources, narrow, block_rows), bf16),
            pltpu.VMEM((ch_size, halves, block_rows, half_width), bf16),
            pltpu.VMEM((ch_size, halves, half_width, columns), bf16),
            pltpu.VMEM(tables.shape, bf16),
            dma((6,)),
            dma((hubs,)),
            dma((seq_size,)),
            dma((hubs,)),
            dma((sources,)),
            dma((seq_size,)),
            dma((hubs,)),
            dma((ch_size, halves)),
            dma((ch_size, halves)),
            pltpu.SemaphoreType.REGULAR((seq_size,)),
            pltpu.SemaphoreType.REGULAR((ch_size,)),
        ],
        compiler_params=pltpu.CompilerParams(
            collective_id=0, has_side_effects=True, vmem_limit_bytes=54500 * 1024
        ),
    )(
        values,
        gates,
        filter_taps,
        skip.reshape(1, width),
        out_weight.reshape(ch_size, halves, half_width, columns),
        jnp.asarray(tables),
    )
    return jnp.concatenate(outs, axis=0)


def local_body(values, gates, filter_taps, skip, out_weight):
    seq_size, ch_size = lax.axis_size("seq"), lax.axis_size("ch")
    block_rows, width = values.shape
    tap_rows = filter_taps.shape[0]
    total = block_rows * seq_size
    sources = min(tap_rows * seq_size, total) // tap_rows
    fits = (
        sources == PAIR * PAIR
        and seq_size % PAIR == 0
        and seq_size >= sources + PAIR
        and width % (sources * TILE) == 0
        and width // sources > TILE
        and width // sources * PAIR % LANES == 0
        and ch_size % 2 == 0
        and block_rows % LANES == 0
        and tap_rows % block_rows == 0
        and sources * block_rows % tap_rows == 0
        and total % tap_rows == 0
        and width // sources * total <= 256 * 1024
    )
    chosen = block_body if fits else body
    return chosen(values, gates, filter_taps, skip, out_weight)


def solution(mesh):
    placed = (P("seq", "ch"), P("seq", "ch"), P("seq", "ch"), P("ch"), P(None, "ch"))
    return jax.shard_map(
        local_body, mesh=mesh, in_specs=placed, out_specs=P("seq", "ch"), check_vma=False
    )
```

```python
import functools
import math

import jax
import jax.numpy as jnp
import numpy as np
from jax import lax
from jax.experimental import pallas as pl
from jax.experimental.pallas import tpu as pltpu
from jax.sharding import PartitionSpec as P

HIGHEST = lax.Precision.HIGHEST
MESH = pl.DeviceIdType.MESH
LANES = 128
TILE = 16
PAIR = 2


def split_length(length):
    leading = 1
    for factor in range(1, math.isqrt(length) + 1):
        if length % factor == 0:
            leading = factor
    return (leading, length // leading)


def phase_table(count_rows, count_cols, modulus):
    row_ids = jnp.arange(count_rows, dtype=jnp.int32)
    col_ids = jnp.arange(count_cols, dtype=jnp.int32)
    wrapped = row_ids[:, None] * col_ids[None, :] % modulus
    phases = 2.0 * math.pi / modulus * wrapped.astype(jnp.float32)
    return (jnp.cos(phases), jnp.sin(phases))


def complex_form(cosine, sine):
    upper = jnp.stack([cosine, -sine], axis=1)
    lower = jnp.stack([sine, cosine], axis=1)
    return jnp.stack([upper, lower], axis=0)


def transform_tables(length):
    rows_lead, rows_tail = split_length(length)
    cos_lead, sin_lead = phase_table(rows_lead, rows_lead, rows_lead)
    cos_tail, sin_tail = phase_table(rows_tail, rows_tail, rows_tail)
    cos_twist, sin_twist = phase_table(rows_lead, rows_tail, length)
    lead_table = jnp.stack([cos_lead, -sin_lead])
    tail_forward = complex_form(cos_tail, -sin_tail)
    tail_inverse = complex_form(cos_tail, sin_tail)
    return (
        lead_table,
        tail_forward,
        tail_inverse,
        cos_twist,
        sin_twist,
        rows_lead,
        rows_tail,
        length,
    )


def twist_rows(section, cosine, sine):
    real_part = section[0] * cosine[None] - section[1] * sine[None]
    imag_part = section[0] * sine[None] + section[1] * cosine[None]
    return jnp.stack([real_part, imag_part])


def forward_rows(rows, tables):
    lead_table, tail_forward, tail_inverse, cos_twist, sin_twist, rows_lead, rows_tail, length = (
        tables
    )
    signal = jnp.concatenate([rows, jnp.zeros_like(rows)], axis=1).reshape(
        rows.shape[0], rows_lead, rows_tail
    )
    section = jnp.einsum("pft,cts->pcfs", lead_table, signal, precision=HIGHEST)
    twisted = twist_rows(section, cos_twist, -sin_twist)
    return jnp.einsum("pgrs,rcfs->pcfg", tail_forward, twisted, precision=HIGHEST)


def inverse_rows(spectrum, tables):
    lead_table, tail_forward, tail_inverse, cos_twist, sin_twist, rows_lead, rows_tail, length = (
        tables
    )
    section = jnp.einsum("pgrs,rcfs->pcfg", tail_inverse, spectrum, precision=HIGHEST)
    twisted = twist_rows(section, cos_twist, sin_twist)
    signal = jnp.einsum("rft,rcfs->cts", lead_table, twisted, precision=HIGHEST) / length
    return signal.reshape(signal.shape[0], length)


def product(left, right):
    real_part = left[0] * right[0] - left[1] * right[1]
    imag_part = left[0] * right[1] + left[1] * right[0]
    return jnp.stack([real_part, imag_part])


def body(values, gates, filter_taps, skip, out_weight):
    block_rows, width = values.shape
    whole_filter = lax.all_gather(filter_taps, "seq", axis=0, tiled=True)
    devices = lax.axis_size("seq")
    narrow = width // devices
    whole_rows = lax.all_to_all(values.T, "seq", split_axis=0, concat_axis=1, tiled=True)
    total_rows = whole_rows.shape[1]
    own_taps = lax.dynamic_slice_in_dim(whole_filter, lax.axis_index("seq") * narrow, narrow, 1).T
    used_taps = min(own_taps.shape[1], total_rows)
    own_taps = own_taps[:, :used_taps]
    taps_rows = jnp.concatenate(
        [own_taps, jnp.zeros((narrow, total_rows - used_taps), jnp.float32)], axis=1
    )
    row_tables = transform_tables(2 * total_rows)
    spectrum = product(forward_rows(whole_rows, row_tables), forward_rows(taps_rows, row_tables))
    convolved_rows = inverse_rows(spectrum, row_tables)[:, :total_rows]
    convolved = lax.all_to_all(convolved_rows, "seq", split_axis=1, concat_axis=0, tiled=True).T
    hidden = (gates * (convolved + skip[None, :] * values)).astype(jnp.bfloat16)
    return jnp.dot(
        lax.all_gather(hidden, "ch", axis=1, tiled=True),
        out_weight,
        preferred_element_type=jnp.float32,
    )


def block_tables():
    size = 2 * LANES
    place = np.arange(size)[:, None]
    odd = 2 * np.arange(LANES)[None, :] + 1
    angle = np.pi / size * (place * odd % (2 * size))
    forward = np.concatenate([np.cos(angle), -np.sin(angle)], axis=1)
    inverse = forward[LANES:].T / LANES

    def two_parts(table, axis):
        high = table.astype(jnp.bfloat16)
        low = (table - high.astype(np.float64)).astype(jnp.bfloat16)
        return np.concatenate([high, low], axis=axis)

    return two_parts(forward, 0), two_parts(inverse, 1)


OUTS = 2


def block_kernel(
    values_hbm,
    gates_hbm,
    taps_hbm,
    skip_hbm,
    weight_hbm,
    tables_hbm,
    out_a,
    out_b,
    values_ref,
    gates_ref,
    taps_ref,
    skip_ref,
    x_out,
    h_out,
    x_in,
    h_in,
    x_tail,
    h_tail,
    x_waves,
    h_waves,
    y_waves,
    y_out,
    y_tail,
    y_in,
    hidden,
    weight,
    tables,
    load_sem,
    x_send,
    x_recv,
    h_send,
    h_recv,
    y_send,
    y_recv,
    g_send,
    g_recv,
    seq_ready,
    ch_ready,
):
    sources, narrow, block_rows = x_out.shape
    seq_size = x_in.shape[0]
    tap_rows = h_out.shape[2]
    ch_size, halves, _, half_width = hidden.shape
    per, pieces = block_rows // LANES, tap_rows // LANES
    hubs, keep = sources + PAIR, narrow - TILE
    early_taps = sources * block_rows // tap_rows
    me, lane_group = lax.axis_index("seq"), lax.axis_index("ch")
    f32, bf16 = jnp.float32, jnp.bfloat16

    loads = [
        pltpu.make_async_copy(source, target, load_sem.at[place])
        for place, (source, target) in enumerate(
            (
                (values_hbm, values_ref),
                (taps_hbm, taps_ref),
                (tables_hbm, tables),
                (gates_hbm, gates_ref),
                (skip_hbm, skip_ref),
                (weight_hbm, weight),
            )
        )
    ]
    for load in loads:
        load.start()

    barrier = pltpu.get_barrier_semaphore()
    for other in range(1, seq_size):
        @pl.when((me < other) & (me < hubs))
        def _():
            pl.semaphore_signal(barrier, inc=1, device_id={"seq": other}, device_id_type=MESH)
    for other in range(1, ch_size):
        @pl.when(lane_group < other)
        def _():
            pl.semaphore_signal(barrier, inc=1, device_id={"ch": other}, device_id_type=MESH)
    earlier = jnp.minimum(me, hubs) + lane_group

    @pl.when(earlier > 0)
    def _():
        pl.semaphore_wait(barrier, earlier)
    for other in range(hubs):
        @pl.when(me > other)
        def _():
            pl.semaphore_signal(
                seq_ready.at[me], inc=1, device_id={"seq": other}, device_id_type=MESH
            )
    for other in range(ch_size - 1):
        @pl.when(lane_group > other)
        def _():
            pl.semaphore_signal(
                ch_ready.at[lane_group], inc=1, device_id={"ch": other}, device_id_type=MESH
            )

    forward, inverse = tables.at[: 4 * LANES], tables.at[4 * LANES :]
    own, rest = pl.ds(0, keep), pl.ds(keep, TILE)

    def transfer(source, target, sends, recvs, to, place):
        return pltpu.make_async_remote_copy(
            source, target, sends.at[to], recvs.at[place],
            device_id={"seq": to}, device_id_type=MESH,
        )

    def tails_of(helper):
        return pl.ds((helper - sources) * PAIR, PAIR)

    def x_copy(to, place, late):
        if to >= sources:
            source, target = x_out.at[tails_of(to), rest], x_tail.at[place]
        elif late:
            source, target = x_out.at[to, own], x_in.at[place, own]
        else:
            source, target = x_out.at[to], x_in.at[place]
        return transfer(source, target, x_send, x_recv, to, place)

    def h_copy(to, place, late):
        if to >= sources:
            source, target = h_out.at[tails_of(to), rest], h_tail.at[place]
        elif late:
            source, target = h_out.at[to, own], h_in.at[place, own]
        else:
            source, target = h_out.at[to], h_in.at[place]
        return transfer(source, target, h_send, h_recv, to, place)

    def y_copy(to, place):
        if to >= sources:
            source, target = y_out.at[to, own], y_in.at[place, own]
        else:
            source, target = y_out.at[to], y_in.at[place]
        return transfer(source, target, y_send, y_recv, to, place)

    def tail_copy(to, helper, place):
        target = y_in.at[pl.ds((helper - sources) * PAIR, PAIR), rest]
        return transfer(y_tail.at[to], target, y_send, y_recv, to, place)

    def ready(to):
        @pl.when(me < to)
        def _():
            pl.semaphore_wait(seq_ready.at[to], 1)

    def send_tails():
        for to in range(sources, hubs):
            pl.semaphore_wait(seq_ready.at[to], 1)
            x_copy(to, me, False).start()
            h_copy(to, me, False).start()

    loads[0].wait()
    x_out[...] = values_ref[...].T.astype(bf16).reshape(x_out.shape)

    @pl.when(me >= sources)
    def _():
        for to in range(hubs):
            if to >= sources:
                ready(to)

            @pl.when(me != to)
            def _():
                x_copy(to, me, True).start()

    loads[1].wait()

    @pl.when(me < sources)
    def _():
        h_out[...] = taps_ref[...].T.astype(bf16).reshape(h_out.shape)
        for to in range(sources):
            ready(to)

            @pl.when(me != to)
            def _():
                x_copy(to, me, False).start()

            @pl.when((me != to) & (me < early_taps))
            def _():
                h_copy(to, me, False).start()

            @pl.when((me != to) & (me >= early_taps))
            def _():
                h_copy(to, me, True).start()

        @pl.when(me >= early_taps)
        def _():
            send_tails()

        x_in[me] = x_out[me]
        h_in[me] = h_out[me]

    loads[2].wait()

    def wait_taps(source, helper):
        late = source >= early_taps
        if helper:
            h_copy(sources, source, late).wait_recv()
        else:
            @pl.when(me != source)
            def _():
                h_copy(0, source, late).wait_recv()

    def wait_values(first, helper):
        for source in range(first, first + PAIR):
            @pl.when(me != source)
            def _():
                x_copy(sources if helper else 0, source, first >= sources).wait_recv()

    def take_taps(source, helper):
        if helper:
            taps, count = h_tail.at[source], PAIR * TILE
        else:
            taps, count = h_in.at[source], keep if source >= early_taps else narrow
        rows = []
        for piece in range(pieces):
            lanes = slice(piece * LANES, (piece + 1) * LANES)
            block = taps[:, :, lanes].reshape(count, LANES) if helper else taps[:count, lanes]
            rows.append(jnp.concatenate([block, block], axis=1))
        table = jnp.concatenate([forward[:LANES], forward[2 * LANES : 3 * LANES]], axis=0)
        waves = jnp.dot(jnp.concatenate(rows, axis=0), table, preferred_element_type=f32)
        h_waves[source * pieces : (source + 1) * pieces, :count] = waves.reshape(
            pieces, count, 2 * LANES
        )

    def take_values(first, helper):
        late = first >= sources
        count = PAIR * TILE if helper else keep if late else narrow
        def piece_of(source, piece):
            lanes = slice(piece * LANES, (piece + 1) * LANES)
            if helper:
                return x_tail[source, :, :, lanes].reshape(count, LANES)
            return x_in[source, :count, lanes]

        before = piece_of(first - 1, per - 1) if first else jnp.zeros((count, LANES), bf16)
        rows = []
        for source in range(first, first + PAIR):
            for piece in range(per):
                here = piece_of(source, piece)
                rows.append(jnp.concatenate([before, here, before, here], axis=1))
                before = here
        waves = jnp.dot(
            jnp.concatenate(rows, axis=0), forward[...], preferred_element_type=f32
        )
        x_waves[first * per : (first + PAIR) * per, :count] = waves.reshape(
            PAIR * per, count, 2 * LANES
        )

    def multiply(first, low, high, fresh, tiles):
        start, count = first * per, PAIR * per

        def one(part, carry):
            rows = pl.ds(pl.multiple_of(part * TILE, TILE), TILE)
            real_lanes, imag_lanes = slice(0, LANES), slice(LANES, 2 * LANES)
            cache = {}

            def x_part(block):
                if block not in cache:
                    cache[block] = (
                        x_waves[block, rows, real_lanes], x_waves[block, rows, imag_lanes]
                    )
                return cache[block]

            sums = [None] * count
            if not fresh:
                sums = [
                    (y_waves[start + spot, rows, real_lanes], y_waves[start + spot, rows, imag_lanes])
                    for spot in range(count)
                ]
            for lag in range(max(0, start - high + 1), start + count - low):
                h_real, h_imag = h_waves[lag, rows, real_lanes], h_waves[lag, rows, imag_lanes]
                for spot in range(count):
                    block = start + spot - lag
                    if not low <= block < high:
                        continue
                    x_real, x_imag = x_part(block)
                    real = x_real * h_real - x_imag * h_imag
                    imag = x_real * h_imag + x_imag * h_real
                    if sums[spot] is not None:
                        real, imag = sums[spot][0] + real, sums[spot][1] + imag
                    sums[spot] = (real, imag)
            for spot in range(count):
                y_waves[start + spot, rows, real_lanes] = sums[spot][0]
                y_waves[start + spot, rows, imag_lanes] = sums[spot][1]
            return carry

        lax.fori_loop(0, tiles, one, 0)

    def give_back(first, helper):
        count = PAIR * TILE if helper else keep if first >= sources else narrow
        waves = y_waves[first * per : (first + PAIR) * per, :count].reshape(
            PAIR * per * count, 2 * LANES
        )
        high = waves.astype(bf16)
        low = (waves - high.astype(f32)).astype(bf16)
        both = jnp.dot(high, inverse[...], preferred_element_type=f32)
        more = jnp.dot(low, inverse[:, :LANES], preferred_element_type=f32)
        convolved = (both[:, :LANES] + both[:, LANES:] + more).astype(bf16)
        for spot in range(PAIR * per):
            to, piece = first + spot // per, spot % per
            lanes = slice(piece * LANES, (piece + 1) * LANES)
            part = convolved[spot * count : (spot + 1) * count]
            if helper:
                y_tail[to, :, :, lanes] = part.reshape(PAIR, TILE, LANES)
            else:
                y_out[to, :count, lanes] = part
        for to in range(first, first + PAIR):
            if to >= hubs:
                pl.semaphore_wait(seq_ready.at[to], 1)
            if not helper:
                @pl.when(me != to)
                def _():
                    y_copy(to, me).start()
            else:
                for which in range(sources, hubs):
                    @pl.when((me == which) & (me != to))
                    def _():
                        tail_copy(to, which, me).start()

    def convolve_own():
        taken = 0
        for first in range(0, sources, PAIR):
            fresh = taken
            while taken < early_taps and taken * tap_rows < (first + PAIR) * block_rows:
                wait_taps(taken, False)
                taken += 1
            wait_values(first, False)
            if not first:
                @pl.when(me < early_taps)
                def _():
                    send_tails()

            for source in range(fresh, taken):
                take_taps(source, False)
            take_values(first, False)
            multiply(first, 0, (first + PAIR) * per, True, narrow // TILE)
            give_back(first, False)
        tiles = keep // TILE
        for source in range(early_taps, sources):
            wait_taps(source, False)
        for source in range(early_taps, sources):
            take_taps(source, False)
        for first in range(sources, seq_size, PAIR):
            multiply(first, 0, sources * per, True, tiles)
        for first in range(sources, seq_size, PAIR):
            wait_values(first, False)
        for first in range(sources, seq_size, PAIR):
            take_values(first, False)
        for first in range(sources, seq_size, PAIR):
            multiply(first, sources * per, (first + PAIR) * per, False, tiles)
            give_back(first, False)

    def convolve_tails():
        for first in range(PAIR, seq_size, PAIR):
            wait_values(first, True)
            if first >= sources:
                take_values(first, True)
        for source in range(early_taps, sources):
            wait_taps(source, True)
            take_taps(source, True)
        wait_values(0, True)
        for source in range(early_taps):
            wait_taps(source, True)
        for first in range(0, sources, PAIR):
            take_values(first, True)
        for source in range(early_taps):
            take_taps(source, True)
        for first in range(seq_size - PAIR, sources - 1, -PAIR):
            multiply(first, 0, (first + PAIR) * per, True, PAIR)
            give_back(first, True)

    @pl.when(me < sources)
    def _():
        convolve_own()
        y_in[me] = y_out[me]

    for which in range(sources, hubs):
        @pl.when(me == which)
        def _():
            tails = slice((which - sources) * PAIR, (which - sources + 1) * PAIR)
            x_tail[which] = x_out[tails, keep:]

    @pl.when((me >= sources) & (me < hubs))
    def _():
        convolve_tails()

    for which in range(sources, hubs):
        @pl.when(me == which)
        def _():
            tails = slice((which - sources) * PAIR, (which - sources + 1) * PAIR)
            y_in[tails, keep:] = y_tail[which]

    partner = lane_group + 1 - 2 * lax.rem(lane_group, 2)
    pairs = ch_size // 2

    def spread(kind, half, slot, to):
        block = hidden.at[slot, half]
        copy = pltpu.make_async_remote_copy(
            block, block, g_send.at[kind, half], g_recv.at[kind, half],
            device_id={"ch": to}, device_id_type=MESH,
        )
        copy.start()
        g_copies.append(copy)
        return copy

    def add_product(half, slot, first=False):
        term = jnp.dot(hidden[slot, half], weight[slot, half], preferred_element_type=f32)
        for place, out in enumerate(outs):
            part = term[place * out_rows : (place + 1) * out_rows]
            out[...] = part if first else out[...] + part

    for other in range(1, ch_size):
        @pl.when(lane_group < other)
        def _():
            pl.semaphore_wait(ch_ready.at[other], 1)

    outs = (out_a, out_b)
    out_rows = out_a.shape[0]
    g_copies, direct, relayed = [], {}, {}
    for load in loads[3:5]:
        load.wait()
    for half in range(halves):
        for part in range(PAIR):
            source = half * PAIR + part

            @pl.when((me != source) & (me < sources))
            def _():
                y_copy(0, source).wait_recv()

            @pl.when(me >= sources)
            def _():
                y_copy(sources, source).wait_recv()

        @pl.when((me >= sources) & (me != sources + half))
        def _():
            tail_copy(sources, sources, sources + half).wait_recv()
        convolved = y_in[half * PAIR : (half + 1) * PAIR].astype(f32).reshape(half_width, block_rows).T
        span = slice(half * half_width, (half + 1) * half_width)
        hidden[lane_group, half] = (
            gates_ref[:, span] * (convolved + skip_ref[:, span] * values_ref[:, span])
        ).astype(bf16)
        for pair in range(1, pairs):
            direct[pair, half] = spread(
                2 * pair - 1, half, lane_group, lax.rem(lane_group + 2 * pair, ch_size)
            )
            if half == halves - 1:
                relayed[pair, half] = spread(
                    2 * pair, half, lane_group, lax.rem(partner + 2 * pair, ch_size)
                )
        direct[0, half] = spread(0, half, lane_group, partner)
    loads[5].wait()
    for half in range(halves):
        add_product(half, lane_group, not half)
    for half in range(halves):
        direct[0, half].wait_recv()
        add_product(half, partner)
        for pair in range(1, pairs):
            slot = lax.rem(lane_group + ch_size - 2 * pair, ch_size)
            direct[pair, half].wait_recv()
            if half < halves - 1:
                relayed[pair, half] = spread(2 * pair, half, slot, partner)
            add_product(half, slot)
    for half in range(halves):
        for pair in range(1, pairs):
            slot = lax.rem(partner + ch_size - 2 * pair, ch_size)
            relayed[pair, half].wait_recv()
            add_product(half, slot)

    for copy in g_copies:
        copy.wait_send()
    for to in range(hubs):
        for late in (False, True):
            @pl.when((me != to) & ((me >= sources) == late))
            def _():
                x_copy(to, me, late).wait_send()

            @pl.when((me != to) & (me < sources) & ((me >= early_taps) == late))
            def _():
                h_copy(to, me, late).wait_send()
    for to in range(seq_size):
        @pl.when((me != to) & (me < sources))
        def _():
            y_copy(to, me).wait_send()

        if to >= sources:
            @pl.when((me != to) & (me >= sources) & (me < hubs))
            def _():
                tail_copy(to, sources, me).wait_send()


def block_body(values, gates, filter_taps, skip, out_weight):
    seq_size, ch_size = lax.axis_size("seq"), lax.axis_size("ch")
    block_rows, width = values.shape
    tap_rows = filter_taps.shape[0]
    total = block_rows * seq_size
    sources = min(tap_rows * seq_size, total) // tap_rows
    narrow, halves, hubs = width // sources, sources // PAIR, sources + PAIR
    half_width = width // halves
    columns = out_weight.shape[1]
    f32, bf16 = jnp.float32, jnp.bfloat16
    hbm = pl.BlockSpec(memory_space=pl.ANY)
    dma = pltpu.SemaphoreType.DMA
    tables = np.concatenate(block_tables(), axis=0)
    outs = pl.pallas_call(
        block_kernel,
        out_shape=[jax.ShapeDtypeStruct((block_rows // OUTS, columns), f32)] * OUTS,
        in_specs=[hbm] * 6,
        out_specs=[pl.BlockSpec(memory_space=pltpu.VMEM)] * OUTS,
        scratch_shapes=[
            pltpu.VMEM((block_rows, width), f32),
            pltpu.VMEM((block_rows, width), f32),
            pltpu.VMEM((tap_rows, width), f32),
            pltpu.VMEM((1, width), f32),
            pltpu.VMEM((sources, narrow, block_rows), bf16),
            pltpu.VMEM((sources, narrow, tap_rows), bf16),
            pltpu.VMEM((seq_size, narrow, block_rows), bf16),
            pltpu.VMEM((sources, narrow, tap_rows), bf16),
            pltpu.VMEM((seq_size, PAIR, TILE, block_rows), bf16),
            pltpu.VMEM((sources, PAIR, TILE, tap_rows), bf16),
            pltpu.VMEM((total // LANES, narrow, 2 * LANES), f32),
            pltpu.VMEM((total // LANES, narrow, 2 * LANES), f32),
            pltpu.VMEM((total // LANES, narrow, 2 * LANES), f32),
            pltpu.VMEM((seq_size, narrow, block_rows), bf16),
            pltpu.VMEM((seq_size, PAIR, TILE, block_rows), bf16),
            pltpu.VMEM((sources, narrow, block_rows), bf16),
            pltpu.VMEM((ch_size, halves, block_rows, half_width), bf16),
            pltpu.VMEM((ch_size, halves, half_width, columns), bf16),
            pltpu.VMEM(tables.shape, bf16),
            dma((6,)),
            dma((hubs,)),
            dma((seq_size,)),
            dma((hubs,)),
            dma((sources,)),
            dma((seq_size,)),
            dma((hubs,)),
            dma((ch_size, halves)),
            dma((ch_size, halves)),
            pltpu.SemaphoreType.REGULAR((seq_size,)),
            pltpu.SemaphoreType.REGULAR((ch_size,)),
        ],
        compiler_params=pltpu.CompilerParams(
            collective_id=0, has_side_effects=True, vmem_limit_bytes=54500 * 1024
        ),
    )(
        values,
        gates,
        filter_taps,
        skip.reshape(1, width),
        out_weight.reshape(ch_size, halves, half_width, columns),
        jnp.asarray(tables),
    )
    return jnp.concatenate(outs, axis=0)


def local_body(values, gates, filter_taps, skip, out_weight):
    seq_size, ch_size = lax.axis_size("seq"), lax.axis_size("ch")
    block_rows, width = values.shape
    tap_rows = filter_taps.shape[0]
    total = block_rows * seq_size
    sources = min(tap_rows * seq_size, total) // tap_rows
    fits = (
        sources == PAIR * PAIR
        and seq_size % PAIR == 0
        and seq_size >= sources + PAIR
        and width % (sources * TILE) == 0
        and width // sources > TILE
        and width // sources * PAIR % LANES == 0
        and ch_size % 2 == 0
        and block_rows % LANES == 0
        and tap_rows % block_rows == 0
        and sources * block_rows % tap_rows == 0
        and total % tap_rows == 0
        and width // sources * total <= 256 * 1024
    )
    chosen = block_body if fits else body
    return chosen(values, gates, filter_taps, skip, out_weight)


def solution(mesh):
    placed = (P("seq", "ch"), P("seq", "ch"), P("seq", "ch"), P("ch"), P(None, "ch"))
    return jax.shard_map(
        local_body, mesh=mesh, in_specs=placed, out_specs=P("seq", "ch"), check_vma=False
    )
```
